8 devices in a mesh: layer: 1 (over z), col: 2 (over y), row: 4 (over x, core).
Axes of the slice: x: 2, y: 2, z: 1, core: 2. Of those that a mesh axis runs over, the one named last changes fastest.
Arguments:
- weight: float32 [1024, 4096], P(('layer', 'row'), 'col')
- grad_in: float32 [1024, 4096], P(('layer', 'row'), 'col')
- mom_first: float32 [1024, 4096], P(('layer', 'row'), 'col')
- mom_second: float32 [1024, 4096], P(('layer', 'row'), 'col')
- stat_left: float32 [1024, 1024], P(('layer', 'row'), 'col')
- stat_right: float32 [4096, 4096], P(('layer', 'row'), 'col')
- basis_left: float32 [1024, 1024], P(('layer', 'row'), 'col')
- basis_right: float32 [4096, 4096], P(('layer', 'row'), 'col')
Outputs:
- output 1: float32 [1024, 4096], P(('layer', 'row'), 'col')
- output 2: float32 [1024, 4096], P(('layer', 'row'), 'col')
- output 3: float32 [1024, 4096], P(('layer', 'row'), 'col')
- output 4: float32 [1024, 1024], P(('layer', 'row'), 'col')
- output 5: float32 [4096, 4096], P(('layer', 'row'), 'col')
All inputs are finite; a program needn't handle non-finite values.
Results may differ from the reference program's by a relative error of at most 0.001.
Values are sent between devices in bfloat16 or wider.
A program may use at most 1 GiB of HBM per device.

```python
import jax
import jax.numpy as jnp
from jax import lax

D = 1024
FF = 4096
STEP = 10
RANK = 16
FACTOR_SIDE = 16

BETA1 = 0.9
BETA2 = 0.9
EPS = 1e-8
LR = 0.1
BIAS_ONE = 1.0 - BETA1 ** STEP
BIAS_TWO = 1.0 - BETA2 ** STEP


def random_basis(base_key, matrix_order):
    sub_keys = jax.random.split(base_key, 5)
    side_b = matrix_order // FACTOR_SIDE
    outer_a = jnp.linalg.qr(jax.random.normal(sub_keys[0], (FACTOR_SIDE, FACTOR_SIDE), jnp.float32))[0]
    outer_b = jnp.linalg.qr(jax.random.normal(sub_keys[1], (side_b, side_b), jnp.float32))[0]
    inner_a = jnp.linalg.qr(jax.random.normal(sub_keys[2], (FACTOR_SIDE, FACTOR_SIDE), jnp.float32))[0]
    inner_b = jnp.linalg.qr(jax.random.normal(sub_keys[3], (side_b, side_b), jnp.float32))[0]
    col_order = jax.random.permutation(sub_keys[4], matrix_order)
    first_kron = jnp.kron(outer_a, outer_b)[:, col_order]
    blocks = first_kron.reshape(matrix_order, FACTOR_SIDE, side_b)
    mixed_basis = jnp.einsum("rst,sp,tq->rpq", blocks, inner_a, inner_b)
    return mixed_basis.reshape(matrix_order, matrix_order)


def setup_inputs(seed: int = 0, part: int = 0) -> dict:
    base_key = jax.random.fold_in(jax.random.key(seed), part)
    sub_keys = jax.random.split(base_key, 12)
    grad_scale = (10.0 / FF) ** 0.5
    noise_part = jax.random.normal(sub_keys[0], (D, FF), jnp.float32)
    left_fac = jax.random.normal(sub_keys[1], (D, RANK), jnp.float32)
    right_fac = jax.random.normal(sub_keys[2], (RANK, FF), jnp.float32)
    low_rank = jnp.dot(left_fac, right_fac) * (3.0 / RANK ** 0.5)
    grad_in = (noise_part + low_rank) * FF ** -0.5
    weight = 0.5 * jax.random.normal(sub_keys[3], (D, FF), jnp.float32)
    mom_first = 0.1 * grad_scale * jax.random.normal(sub_keys[4], (D, FF), jnp.float32)
    mom_second = 0.1 * grad_scale ** 2 * (0.25 + jax.random.normal(sub_keys[5], (D, FF), jnp.float32) ** 2)
    stat_fac_left = jax.random.normal(sub_keys[6], (D, RANK), jnp.float32)
    stat_left = 0.5 * ((9.0 / RANK) * jnp.dot(stat_fac_left, stat_fac_left.T) + jnp.eye(D, dtype=jnp.float32))
    stat_fac_right = jax.random.normal(sub_keys[7], (RANK, FF), jnp.float32)
    stat_right = 0.5 * (D / FF) * ((9.0 / RANK) * jnp.dot(stat_fac_right.T, stat_fac_right) + jnp.eye(FF, dtype=jnp.float32))
    basis_left = random_basis(sub_keys[8], D)
    basis_right = random_basis(sub_keys[9], FF)
    return {"weight": weight, "grad_in": grad_in, "mom_first": mom_first, "mom_second": mom_second, "stat_left": stat_left, "stat_right": stat_right, "basis_left": basis_left, "basis_right": basis_right}


def reference(weight, grad_in, mom_first, mom_second, stat_left, stat_right, basis_left, basis_right):
    highest = lax.Precision.HIGHEST
    new_left = BETA2 * stat_left + (1.0 - BETA2) * jnp.dot(grad_in, grad_in.T, precision=highest, preferred_element_type=jnp.float32)
    new_right = BETA2 * stat_right + (1.0 - BETA2) * jnp.dot(grad_in.T, grad_in, precision=highest, preferred_element_type=jnp.float32)
    left_bf = basis_left.astype(jnp.bfloat16)
    right_bf = basis_right.astype(jnp.bfloat16)
    inner_rot = jnp.dot(grad_in.astype(jnp.bfloat16), right_bf, preferred_element_type=jnp.float32).astype(jnp.bfloat16)
    rotated = jnp.dot(left_bf.T, inner_rot, preferred_element_type=jnp.float32)
    new_first = BETA1 * mom_first + (1.0 - BETA1) * rotated
    new_second = BETA2 * mom_second + (1.0 - BETA2) * rotated * rotated
    direction = (new_first / BIAS_ONE) / (jnp.sqrt(new_second / BIAS_TWO) + EPS)
    back_inner = jnp.dot(left_bf, direction.astype(jnp.bfloat16), preferred_element_type=jnp.float32).astype(jnp.bfloat16)
    step_update = jnp.dot(back_inner, right_bf.T, preferred_element_type=jnp.float32)
    new_weight = weight - LR * step_update
    return (new_weight, new_first, new_second, new_left, new_right)
```

```python
import jax
import jax.numpy as jnp
from jax import lax
from jax.sharding import PartitionSpec as P

BETA1 = 0.9
BETA2 = 0.9
EPS = 1e-8
LR = 0.1
STEP = 10
BIAS_ONE = 1.0 - BETA1 ** STEP
BIAS_TWO = 1.0 - BETA2 ** STEP


def _pairs(move, keep=None):
    pairs = []
    for y in range(2):
        for x in range(2):
            for c in range(2):
                if keep is None or keep(y, x):
                    ny, nx, nc = move(y, x, c)
                    pairs.append((4 * y + 2 * x + c, 4 * ny + 2 * nx + nc))
    return pairs


PAIRS_X = _pairs(lambda y, x, c: (y, 1 - x, c))
PAIRS_Y = _pairs(lambda y, x, c: (1 - y, x, c))
PAIRS_CORE = _pairs(lambda y, x, c: (y, x, 1 - c))
PAIRS_Y_DIAG_OFF = _pairs(lambda y, x, c: (1 - y, x, c), lambda y, x: x == y)
PAIRS_Y_OFF_DIAG = _pairs(lambda y, x, c: (1 - y, x, c), lambda y, x: x != y)
PAIRS_X_DIAG_OFF = _pairs(lambda y, x, c: (y, 1 - x, c), lambda y, x: x == y)
PAIRS_CROSS = _pairs(lambda y, x, c: (1 - y, 1 - x, c), lambda y, x: x != y)


def _send(value, pairs):
    return lax.ppermute(value, ("col", "row"), pairs)


def solution(mesh):
    tile_spec = P(("layer", "row"), "col")
    highest = lax.Precision.HIGHEST
    contract_rows = (((0,), (0,)), ((), ()))
    contract_cols = (((1,), (1,)), ((), ()))
    f32, bf16 = jnp.float32, jnp.bfloat16

    def local_step(weight, grad_in, mom_first, mom_second, stat_left, stat_right, basis_left, basis_right):
        y, r = lax.axis_index("col"), lax.axis_index("row")
        x, c = r // 2, r % 2
        on_diag = x == y
        half = grad_in.shape[1] // 2
        rows = grad_in.shape[0]

        def mine(array):
            return lax.dynamic_slice_in_dim(array, c * half, half, 1)

        def theirs(array):
            return lax.dynamic_slice_in_dim(array, (1 - c) * half, half, 1)

        def place(own, other):
            return jnp.where(c == 0, jnp.concatenate([own, other], 1), jnp.concatenate([other, own], 1))

        g0 = grad_in
        g2 = _send(g0, PAIRS_X)
        g1 = _send(g0, PAIRS_CORE)
        g3 = _send(g2, PAIRS_CORE)
        pieces = [g0, g1, g2, g3]
        left = [jnp.where(on_diag, mine(p), _send(mine(p), PAIRS_Y_DIAG_OFF)) for p in pieces]
        left_bf = [p.astype(bf16) for p in left]
        part_bf = [_send(p, PAIRS_CORE) for p in left_bf]
        part_bf = [part_bf[1], part_bf[0], part_bf[3], part_bf[2]]

        right_bf = basis_right.astype(bf16)
        right_mine, right_theirs = mine(right_bf), theirs(right_bf)
        right_part = _send(right_theirs, PAIRS_CORE)

        q0 = basis_left.astype(bf16)
        q2 = _send(q0, PAIRS_X)
        qa = jnp.concatenate([q0, q2], 0)
        qb = _send(qa, PAIRS_Y)
        qm = jnp.stack([jnp.where(on_diag, qa, qb), jnp.where(on_diag, qb, qa)])
        qp = _send(qm, PAIRS_CORE)
        cols = []
        for k in range(2):
            block = jnp.concatenate([qm[k, :rows], qp[k, :rows], qm[k, rows:], qp[k, rows:]], 0)
            swapped = jnp.concatenate([block[:, rows:], block[:, :rows]], 1)
            cols.append(jnp.where(c == 0, block, swapped))
        left_all = jnp.concatenate(cols, 1)

        def inner(k):
            a = jnp.concatenate([left_bf[k], left_bf[k + 1]], 0)
            b = jnp.concatenate([part_bf[k], part_bf[k + 1]], 0)
            return jnp.dot(a, right_mine, preferred_element_type=f32) + jnp.dot(b, right_part, preferred_element_type=f32)

        far = _send(inner(2), PAIRS_X)
        h_own = (inner(0) + far).astype(bf16)
        h_far = _send(h_own, PAIRS_X)
        h_all = jnp.concatenate([h_own, h_far], 0)
        rotated = lax.dot_general(left_all[:, : 2 * rows], h_all, contract_rows, preferred_element_type=f32)

        first = jnp.concatenate([mine(mom_first), _send(theirs(mom_first), PAIRS_CORE)], 0)
        second = jnp.concatenate([mine(mom_second), _send(theirs(mom_second), PAIRS_CORE)], 0)
        new_first = BETA1 * first + (1.0 - BETA1) * rotated
        new_second = BETA2 * second + (1.0 - BETA2) * rotated * rotated
        direction = ((new_first / BIAS_ONE) / (jnp.sqrt(new_second / BIAS_TWO) + EPS)).astype(bf16)
        dir_all = jnp.concatenate([direction, _send(direction, PAIRS_X)], 0)
        back = jnp.dot(left_all, dir_all, preferred_element_type=f32).astype(bf16)
        back_p = _send(back, PAIRS_CORE)
        back_p = jnp.concatenate([back_p[rows : 2 * rows], back_p[:rows], back_p[3 * rows :], back_p[2 * rows : 3 * rows]], 0)

        def update(lo):
            a, b = back[lo : lo + 2 * rows], back_p[lo : lo + 2 * rows]
            return lax.dot_general(a, right_mine, contract_cols, preferred_element_type=f32) + lax.dot_general(
                b, right_theirs, contract_cols, preferred_element_type=f32
            )

        up_far = update(2 * rows)
        up_near = update(0)
        total = (
            jnp.where(on_diag, up_near, 0.0)
            + _send(up_near, PAIRS_Y_OFF_DIAG)
            + _send(up_far, PAIRS_X_DIAG_OFF)
            + _send(up_far, PAIRS_CROSS)
        )
        new_weight = weight - LR * place(total[:rows], _send(total[rows:], PAIRS_CORE))
        out_first = place(new_first[:rows], _send(new_first[rows:], PAIRS_CORE))
        out_second = place(new_second[:rows], _send(new_second[rows:], PAIRS_CORE))

        stat = [lax.dot_general(p, g0, contract_cols, precision=highest, preferred_element_type=f32).T for p in pieces]
        near = place(stat[0], stat[1])
        away = place(stat[2], stat[3])
        got = _send(jnp.where(on_diag, away, near), PAIRS_Y)
        new_left = BETA2 * stat_left + (1.0 - BETA2) * (jnp.where(on_diag, near, away) + got)
        wide = jnp.concatenate(pieces, 0)
        tall = jnp.concatenate(left, 0)
        right_sum = lax.dot_general(tall, wide, contract_rows, precision=highest, preferred_element_type=f32)
        new_right = BETA2 * stat_right + (1.0 - BETA2) * right_sum
        return new_weight, out_first, out_second, new_left, new_right

    return jax.shard_map(local_step, mesh=mesh, in_specs=(tile_spec,) * 8, out_specs=(tile_spec,) * 5, check_vma=False)
```

```python
import functools

import jax
import jax.numpy as jnp
from jax import lax
from jax.experimental import pallas as pl
from jax.experimental.pallas import tpu as pltpu
from jax.sharding import PartitionSpec as P

BETA1 = 0.9
BETA2 = 0.9
EPS = 1e-8
LR = 0.1
STEP = 10
BIAS_ONE = 1.0 - BETA1 ** STEP
BIAS_TWO = 1.0 - BETA2 ** STEP

MESH = pl.DeviceIdType.MESH
F32, BF16 = jnp.float32, jnp.bfloat16
CHUNKS = 4
COPIES = 64


def _step(
    w_ref, g_ref, m_ref, v_ref, l_ref, r_ref, ql_ref, qr_ref,
    wo_ref, mo_ref, vo_ref, lo_ref, ro_ref,
    gat, acc, gbf, qrx, qro, part, precv, hbuf, qlb, qlt, mt, vt, wt, nbuf, kbuf, urecv, lbuf, qstage,
    ssem, rsem, lsem,
):
    y, r = lax.axis_index("col"), lax.axis_index("row")
    x, c = r // 2, r % 2
    diag = x == y
    off = x != y
    sel = jnp.where(diag, 0, 1)
    own, far = 2 * x, 2 * (1 - x)
    rx = 2 * (1 - x) + c
    rp = 2 * x + 1 - c
    rxp = 2 * (1 - x) + 1 - c
    mine = pl.ds(pl.multiple_of(c * 1024, 1024), 1024)
    other = pl.ds(pl.multiple_of((1 - c) * 1024, 1024), 1024)
    to_x, to_core, to_y, to_cross = (0, y, rx), (0, y, rp), (0, 1 - y, r), (0, 1 - y, rx)

    used = [0]
    local_used = [0]

    def remote(src, dst, dev):
        n = used[0]
        used[0] += 1
        return pltpu.make_async_remote_copy(
            src_ref=src, dst_ref=dst, send_sem=ssem.at[n], recv_sem=rsem.at[n], device_id=dev, device_id_type=MESH
        )

    def local(src, dst):
        n = local_used[0]
        local_used[0] += 1
        return pltpu.make_async_copy(src, dst, lsem.at[n])

    ld_g = local(g_ref, gat.at[0, r])
    ld_qr = local(qr_ref, acc)
    ld_ql = local(ql_ref, qstage)
    ld_m = local(m_ref.at[:, mine], mt.at[c])
    ld_v = local(v_ref.at[:, mine], vt.at[c])
    ld_w = local(w_ref.at[:, mine], wt.at[c])
    ld_l = local(l_ref, lbuf.at[0])
    for cp in (ld_ql, ld_qr, ld_g, ld_m, ld_v, ld_w, ld_l):
        cp.start()

    barrier = pltpu.get_barrier_semaphore()
    for dev in (to_x, to_core, to_y, to_cross):
        pl.semaphore_signal(barrier, inc=1, device_id=dev, device_id_type=MESH)
    pl.semaphore_wait(barrier, 4)

    def rows(k):
        return pl.ds(64 * k, 64)

    gx = [remote(g_ref.at[rows(k), :], gat.at[0, r, rows(k), :], to_x) for k in range(CHUNKS)]
    gp = remote(g_ref, gat.at[0, r], to_core)
    sm = remote(m_ref.at[:, other], mt.at[c], to_core)
    sv = remote(v_ref.at[:, other], vt.at[c], to_core)
    sw = remote(w_ref.at[:, other], wt.at[c], to_core)
    qcol = pl.ds(pl.multiple_of(y * 512, 512), 512)
    qx = remote(qlb.at[r, :, qcol], qlb.at[r, :, qcol], to_x)
    qya = remote(qlb.at[r, :, qcol], qlb.at[r, :, qcol], to_y)
    qyb = remote(qlb.at[rx, :, qcol], qlb.at[rx, :, qcol], to_y)
    qpa = remote(qlb.at[r], qlb.at[r], to_core)
    qpb = remote(qlb.at[rx], qlb.at[rx], to_core)
    qrp = remote(qro, qrx.at[c], to_core)
    gb = remote(gbf.at[:, :, mine], gbf.at[:, :, mine], to_y)
    fb = remote(gbf.at[:, :, mine], gbf.at[:, :, mine], to_core)
    gf = [remote(gat.at[0, rx, rows(k), :], gat.at[0, rx, rows(k), :], to_core) for k in range(CHUNKS)]
    y2 = [remote(gat.at[0, rx, rows(k), mine], gat.at[1, rx, rows(k), mine], to_y) for k in range(CHUNKS)]
    y3 = [remote(gat.at[0, rxp, rows(k), mine], gat.at[1, rxp, rows(k), mine], to_y) for k in range(CHUNKS)]
    f2 = [remote(gat.at[1, rx, rows(k), mine], gat.at[1, rx, rows(k), mine], to_core) for k in range(CHUNKS)]
    f3 = [remote(gat.at[1, rxp, rows(k), mine], gat.at[1, rxp, rows(k), mine], to_core) for k in range(CHUNKS)]
    ya = remote(gat.at[0, pl.ds(own, 2), :, mine], gat.at[1, pl.ds(own, 2), :, mine], to_y)

    def pslot(base, k):
        return part.at[base + k // 2, pl.ds(128 * (k % 2), 128), :]

    px = [remote(pslot(0, k), precv.at[k], to_x) for k in range(CHUNKS)]
    hx = [remote(hbuf.at[pl.ds(own, 2), rows(k), :], hbuf.at[pl.ds(own, 2), rows(k), :], to_x) for k in range(CHUNKS)]
    half = pl.ds(pl.multiple_of(x * 512, 512), 512)
    nx = [remote(nbuf.at[j, half, :], nbuf.at[j, half, :], to_x) for j in range(CHUNKS)]
    kp = [remote(kbuf.at[c, :, pl.ds(256 * j, 256)], kbuf.at[c, :, pl.ds(256 * j, 256)], to_core) for j in range(CHUNKS)]
    mo = remote(mt.at[1 - c], mo_ref.at[:, mine], to_core)
    vo = remote(vt.at[1 - c], vo_ref.at[:, mine], to_core)
    wo = remote(wt.at[1 - c], wo_ref.at[:, mine], to_core)
    order = [1 - c, c]
    ux = [remote(part.at[far + i], urecv.at[0, i], to_x) for i in order]
    uy = [remote(part.at[own + i], urecv.at[0, i], to_y) for i in order]
    uc = [remote(part.at[far + i], urecv.at[1, i], to_cross) for i in order]
    lx = remote(lbuf.at[1], lbuf.at[2], to_y)

    for cp in gx:
        cp.start()
    gp.start()
    ld_ql.wait()
    qlb[r, :, qcol] = qstage[...].astype(BF16)
    qya.start()
    qx.start()

    ld_qr.wait()

    def to_bf(t, carry):
        span = pl.ds(pl.multiple_of(t * 128, 128), 128)
        qro[span, :] = acc[span, other].astype(BF16)
        qrx[c, span, :] = acc[span, mine].astype(BF16)
        return carry

    lax.fori_loop(0, 8, to_bf, 0)
    qrp.start()
    ld_r = local(r_ref, acc)
    ld_r.start()

    ld_g.wait()
    gp.wait_recv()

    @pl.when(diag)
    def _():
        def cast(t, carry):
            span = pl.ds(pl.multiple_of(t * 64, 64), 64)
            for i in range(2):
                gbf[i, span, :] = gat[0, own + i, span, :].astype(BF16)
            return carry

        lax.fori_loop(0, 4, cast, 0)
        gb.start()

    sm.start()
    sv.start()
    sw.start()

    qrp.wait_recv()

    def inner(load, store):
        top, low = load(0), load(1)
        lhs = jnp.concatenate([top, low], 0)

        def cols(t, carry):
            span = pl.ds(pl.multiple_of(t * 256, 256), 256)
            value = jnp.dot(lhs[:, :1024], qrx[0, :, span], preferred_element_type=F32)
            value += jnp.dot(lhs[:, 1024:], qrx[1, :, span], preferred_element_type=F32)
            store(span, value)
            return carry

        lax.fori_loop(0, 4, cols, 0)

    def send_part(k):
        def store(span, value):
            part[k // 2, pl.ds(128 * (k % 2), 128), span] = value

        inner(lambda i: gat[sel, far + i, rows(k), :].astype(BF16), store)
        px[k].start()

    def relay(k):
        @pl.when(off)
        def _():
            y2[k].wait_recv()
            f2[k].start()
            y3[k].wait_recv()
            f3[k].start()
            f2[k].wait_recv()
            f3[k].wait_recv()

    for k in range(CHUNKS):
        gx[k].wait_recv()
        gf[k].start()

        @pl.when(diag)
        def _():
            y2[k].start()

        gf[k].wait_recv()

        @pl.when(diag)
        def _():
            y3[k].start()

        if k == 1:

            @pl.when(off)
            def _():
                gb.wait_recv()
                fb.start()

    qx.wait_recv()
    qyb.start()

    @pl.when(diag)
    def _():
        ya.start()

    @pl.when(off)
    def _():
        fb.wait_recv()

    def stat_right(base, t, last):
        lane = pl.ds(pl.multiple_of(c * 1024 + t * 256, 256), 256)
        tall = jnp.concatenate([gat[sel, base, :, lane], gat[sel, base + 1, :, lane]], 0).T
        span = pl.ds(pl.multiple_of(t * 256, 256), 256)

        def cols(n, carry):
            at = pl.ds(pl.multiple_of(n * 256, 256), 256)
            wide = jnp.concatenate([gat[0, base, :, at], gat[0, base + 1, :, at]], 0)
            value = jnp.dot(tall, wide, precision=lax.Precision.HIGHEST, preferred_element_type=F32)
            prev = acc[span, at]
            if not last:
                prev = BETA2 * prev
            acc[span, at] = prev + (1.0 - BETA2) * value
            return carry

        lax.fori_loop(0, 8, cols, 0)

    def stat_left(k):
        slot = jnp.where(y == k, 0, 1)
        for i in range(2):
            value = lax.dot_general(
                gat[0, r], gat[0, 2 * k + i], (((1,), (1,)), ((), ())), precision=lax.Precision.HIGHEST, preferred_element_type=F32
            )
            at = pl.ds(256 * i, 256)

            @pl.when(slot == 0)
            def _():
                lbuf[0, :, at] = BETA2 * lbuf[0, :, at] + (1.0 - BETA2) * value

            @pl.when(slot == 1)
            def _():
                lbuf[1, :, at] = value

    ld_r.wait()
    ld_l.wait()
    for k in range(CHUNKS):
        relay(k)
        send_part(k)

    def own_part(k):
        def store(span, value):
            part[2 + k // 2, pl.ds(128 * (k % 2), 128), span] = value

        inner(lambda i: gbf[i, rows(k), :], store)

    for k in range(CHUNKS):
        own_part(k)
    for k in range(CHUNKS):
        if k < 3:
            stat_right(far, k, False)
        px[k].wait_recv()
        for i in range(2):
            at = pl.ds(128 * (k % 2) + 64 * i, 64)
            hbuf[own + i, rows(k), :] = (part[2 + k // 2, at, :] + precv[k, pl.ds(64 * i, 64), :]).astype(BF16)
        hx[k].start()

    qya.wait_recv()
    qyb.wait_recv()
    qpa.start()
    qpb.start()
    qpa.wait_recv()
    qpb.wait_recv()

    def turn(t, carry):
        lane = pl.ds(pl.multiple_of(x * 512 + t * 128, 128), 128)
        for p in range(4):
            qlt[pl.ds(pl.multiple_of(t * 128, 128), 128), pl.ds(256 * p, 256)] = qlb[p, :, lane].astype(F32).T.astype(BF16)
        return carry

    lax.fori_loop(0, 4, turn, 0)
    stat_right(far, 3, False)
    ld_m.wait()
    ld_v.wait()
    ld_w.wait()
    sm.wait_recv()
    sv.wait_recv()
    sw.wait_recv()
    for k in range(CHUNKS):
        hx[k].wait_recv()

    for j in range(CHUNKS):
        at = pl.ds(256 * j, 256)
        for i in range(2):
            rot = jnp.zeros((256, 256), F32)
            for p in range(4):
                rot += jnp.dot(qlt[pl.ds(256 * i, 256), pl.ds(256 * p, 256)], hbuf[p, :, at], preferred_element_type=F32)
            first = BETA1 * mt[i, :, at] + (1.0 - BETA1) * rot
            second = BETA2 * vt[i, :, at] + (1.0 - BETA2) * rot * rot
            mt[i, :, at] = first
            vt[i, :, at] = second
            step = (first / BIAS_ONE) / (jnp.sqrt(second / BIAS_TWO) + EPS)
            nbuf[j, pl.ds(pl.multiple_of(x * 512 + 256 * i, 256), 256), :] = step.astype(BF16)
        nx[j].start()

    st_m = local(mt.at[c], mo_ref.at[:, mine])
    st_v = local(vt.at[c], vo_ref.at[:, mine])
    st_m.start()
    st_v.start()
    mo.start()
    vo.start()

    stat_left(0)
    stat_left(1)
    lx.start()

    def back(j):
        at = pl.ds(256 * j, 256)
        nx[j].wait_recv()

        def strip(p, carry):
            span = pl.ds(pl.multiple_of(p * 256, 256), 256)
            kbuf[c, span, at] = jnp.dot(qlb[p], nbuf[j], preferred_element_type=F32).astype(BF16)
            return carry

        lax.fori_loop(0, 4, strip, 0)
        kp[j].start()

    def update(p, lo, first):
        span = pl.ds(pl.multiple_of(p * 256, 256), 256)
        at = pl.ds(lo, 512)

        def cols(t, carry):
            lane = pl.ds(pl.multiple_of(t * 256, 256), 256)
            nt = (((1,), (1,)), ((), ()))
            value = lax.dot_general(kbuf[c, span, at], qrx[c, lane, at], nt, preferred_element_type=F32)
            value += lax.dot_general(kbuf[1 - c, span, at], qro[lane, at], nt, preferred_element_type=F32)
            part[p, :, lane] = value if first else part[p, :, lane] + value
            return carry

        lax.fori_loop(0, 4, cols, 0)

    for k in range(CHUNKS):
        px[k].wait_send()
    back(0)
    back(1)
    kp[0].wait_recv()
    kp[1].wait_recv()
    for i in range(4):
        update(i, 0, True)
    back(2)
    back(3)
    kp[2].wait_recv()
    kp[3].wait_recv()
    for n in range(2):
        update(far + order[n], 512, False)

        @pl.when(diag)
        def _():
            ux[n].start()

        @pl.when(off)
        def _():
            uc[n].start()

        update(own + order[n], 512, False)

        @pl.when(off)
        def _():
            uy[n].start()

    @pl.when(off)
    def _():
        ya.wait_recv()

    st_r = []
    for t in range(4):
        stat_right(own, t, True)
        cp = local(acc.at[pl.ds(256 * t, 256), :], ro_ref.at[pl.ds(256 * t, 256), :])
        cp.start()
        st_r.append(cp)
    lx.wait_recv()
    lbuf[0] = lbuf[0] + (1.0 - BETA2) * lbuf[2]
    st_l = local(lbuf.at[0], lo_ref)
    st_l.start()

    for n in range(2):
        i = order[n]

        @pl.when(diag)
        def _():
            uy[n].wait_recv()
            wt[i] = wt[i] - LR * (part[own + i] + urecv[0, i])

        @pl.when(off)
        def _():
            ux[n].wait_recv()
            uc[n].wait_recv()
            wt[i] = wt[i] - LR * (urecv[0, i] + urecv[1, i])

        if n == 0:
            wo.start()
        else:
            st_w = local(wt.at[c], wo_ref.at[:, mine])
            st_w.start()

    for cp in [*gx, gp, sm, sv, sw, qx, qya, qyb, qpa, qpb, qrp, *gf, *hx, *nx, *kp, lx]:
        cp.wait_send()

    @pl.when(diag)
    def _():
        for cp in [gb, *y2, *y3, ya, *ux]:
            cp.wait_send()

    @pl.when(off)
    def _():
        for cp in [fb, *f2, *f3, *uy, *uc]:
            cp.wait_send()

    for cp in (mo, vo, wo):
        cp.wait()
    for cp in (st_m, st_v, st_l, st_w, *st_r):
        cp.wait()


def solution(mesh):
    tile_spec = P(("layer", "row"), "col")

    def local_step(weight, grad_in, mom_first, mom_second, stat_left, stat_right, basis_left, basis_right):
        like = lambda a: jax.ShapeDtypeStruct(a.shape, a.dtype)
        return pl.pallas_call(
            _step,
            out_shape=(like(weight), like(mom_first), like(mom_second), like(stat_left), like(stat_right)),
            in_specs=[pl.BlockSpec(memory_space=pl.ANY)] * 8,
            out_specs=(pl.BlockSpec(memory_space=pl.ANY),) * 5,
            scratch_shapes=[
                pltpu.VMEM((2, 4, 256, 2048), F32),
                pltpu.VMEM((1024, 2048), F32),
                pltpu.VMEM((2, 256, 2048), BF16),
                pltpu.VMEM((2, 1024, 1024), BF16),
                pltpu.VMEM((1024, 1024), BF16),
                pltpu.VMEM((4, 256, 1024), F32),
                pltpu.VMEM((4, 128, 1024), F32),
                pltpu.VMEM((4, 256, 1024), BF16),
                pltpu.VMEM((4, 256, 1024), BF16),
                pltpu.VMEM((512, 1024), BF16),
                pltpu.VMEM((2, 256, 1024), F32),
                pltpu.VMEM((2, 256, 1024), F32),
                pltpu.VMEM((2, 256, 1024), F32),
                pltpu.VMEM((4, 1024, 256), BF16),
                pltpu.VMEM((2, 1024, 1024), BF16),
                pltpu.VMEM((2, 2, 256, 1024), F32),
                pltpu.VMEM((3, 256, 512), F32),
                pltpu.VMEM((256, 512), F32),
                pltpu.SemaphoreType.DMA((COPIES,)),
                pltpu.SemaphoreType.DMA((COPIES,)),
                pltpu.SemaphoreType.DMA((24,)),
            ],
            compiler_params=pltpu.CompilerParams(collective_id=0, has_side_effects=True, vmem_limit_bytes=67043328),
        )(weight, grad_in, mom_first, mom_second, stat_left, stat_right, basis_left, basis_right)

    return jax.shard_map(local_step, mesh=mesh, in_specs=(tile_spec,) * 8, out_specs=(tile_spec,) * 5, check_vma=False)
```

```python
import functools

import jax
import jax.numpy as jnp
from jax import lax
from jax.experimental import pallas as pl
from jax.experimental.pallas import tpu as pltpu
from jax.sharding import PartitionSpec as P

BETA1 = 0.9
BETA2 = 0.9
EPS = 1e-8
LR = 0.1
STEP = 10
BIAS_ONE = 1.0 - BETA1 ** STEP
BIAS_TWO = 1.0 - BETA2 ** STEP

MESH = pl.DeviceIdType.MESH
F32, BF16 = jnp.float32, jnp.bfloat16
CHUNKS = 4
COPIES = 80
GRANT = 51800000


def _step(
    w_ref, g_ref, m_ref, v_ref, l_ref, r_ref, ql_ref, qr_ref,
    wo, mo, vo, lo, acc,
    gat, qrx, qro, part, precv, hbuf, qlb, qlt, mt, vt, wt, nbuf, kbuf, urecv, lbuf,
    ssem, rsem, lsem,
):
    y, r = lax.axis_index("col"), lax.axis_index("row")
    x, c = r // 2, r % 2
    diag = x == y
    off = x != y
    sel = jnp.where(diag, 0, 1)
    own, far = 2 * x, 2 * (1 - x)
    rx = 2 * (1 - x) + c
    rp = 2 * x + 1 - c
    rxp = 2 * (1 - x) + 1 - c
    mine = pl.ds(pl.multiple_of(c * 1024, 1024), 1024)
    other = pl.ds(pl.multiple_of((1 - c) * 1024, 1024), 1024)
    to_x, to_core, to_y, to_cross = (0, y, rx), (0, y, rp), (0, 1 - y, r), (0, 1 - y, rx)

    nt = (((1,), (1,)), ((), ()))
    used = [0]
    local_used = [0]

    def remote(src, dst, dev):
        n = used[0]
        used[0] += 1
        return pltpu.make_async_remote_copy(
            src_ref=src, dst_ref=dst, send_sem=ssem.at[n], recv_sem=rsem.at[n], device_id=dev, device_id_type=MESH
        )

    def local(src, dst):
        n = local_used[0]
        local_used[0] += 1
        return pltpu.make_async_copy(src, dst, lsem.at[n])

    ld_g = local(g_ref, gat.at[0, r])
    ld_qr = local(qr_ref, acc)
    ld_ql = local(ql_ref, lo)
    ld_m = local(m_ref.at[:, mine], mo.at[:, mine])
    ld_v = local(v_ref.at[:, mine], vo.at[:, mine])
    ld_w = local(w_ref.at[:, mine], wo.at[:, mine])
    for cp in (ld_ql, ld_qr, ld_g, ld_m, ld_v, ld_w):
        cp.start()

    barrier = pltpu.get_barrier_semaphore()
    for dev in (to_x, to_core, to_y, to_cross):
        pl.semaphore_signal(barrier, inc=1, device_id=dev, device_id_type=MESH)
    pl.semaphore_wait(barrier, 4)

    def rows(k):
        return pl.ds(64 * k, 64)

    gx = [remote(g_ref.at[rows(k), :], gat.at[0, r, rows(k), :], to_x) for k in range(CHUNKS)]
    gp = remote(g_ref, gat.at[0, r], to_core)
    sm = remote(m_ref.at[:, other], mt, to_core)
    sv = remote(v_ref.at[:, other], vt, to_core)
    sw = remote(w_ref.at[:, other], wt, to_core)
    qcol = pl.ds(pl.multiple_of(y * 512, 512), 512)
    qx = remote(qlb.at[r, :, qcol], qlb.at[r, :, qcol], to_x)
    qya = remote(qlb.at[r, :, qcol], qlb.at[r, :, qcol], to_y)
    qyb = remote(qlb.at[rx, :, qcol], qlb.at[rx, :, qcol], to_y)
    qpa = remote(qlb.at[r], qlb.at[r], to_core)
    qpb = remote(qlb.at[rx], qlb.at[rx], to_core)
    qrp = remote(qro, qrx.at[c], to_core)
    gb = [remote(kbuf.at[c, pl.ds(0, 2), rows(k), :], kbuf.at[c, pl.ds(0, 2), rows(k), :], to_y) for k in range(CHUNKS)]
    fb = [remote(kbuf.at[c, pl.ds(0, 2), rows(k), :], kbuf.at[c, pl.ds(0, 2), rows(k), :], to_core) for k in range(CHUNKS)]
    gf = [remote(gat.at[0, rx, rows(k), :], gat.at[0, rx, rows(k), :], to_core) for k in range(CHUNKS)]
    y2 = [remote(gat.at[0, rx, rows(k), mine], gat.at[1, rx, rows(k), mine], to_y) for k in range(CHUNKS)]
    y3 = [remote(gat.at[0, rxp, rows(k), mine], gat.at[1, rxp, rows(k), mine], to_y) for k in range(CHUNKS)]
    f2 = [remote(gat.at[1, rx, rows(k), mine], gat.at[1, rx, rows(k), mine], to_core) for k in range(CHUNKS)]
    f3 = [remote(gat.at[1, rxp, rows(k), mine], gat.at[1, rxp, rows(k), mine], to_core) for k in range(CHUNKS)]
    ya = remote(gat.at[0, pl.ds(own, 2), :, mine], gat.at[1, pl.ds(own, 2), :, mine], to_y)

    def pslot(base, k):
        return part.at[base + k // 2, pl.ds(128 * (k % 2), 128), :]

    px = [remote(pslot(0, k), precv.at[k], to_x) for k in range(CHUNKS)]
    hx = [remote(hbuf.at[pl.ds(own, 2), rows(k), :], hbuf.at[pl.ds(own, 2), rows(k), :], to_x) for k in range(CHUNKS)]
    half = pl.ds(pl.multiple_of(x * 512, 512), 512)
    nx = [remote(nbuf.at[j, half, :], nbuf.at[j, half, :], to_x) for j in range(CHUNKS)]
    kp = [remote(kbuf.at[c, :, :, pl.ds(256 * j, 256)], kbuf.at[c, :, :, pl.ds(256 * j, 256)], to_core) for j in range(CHUNKS)]
    om = remote(mt, mo.at[:, mine], to_core)
    ov = remote(vt, vo.at[:, mine], to_core)
    order = [1 - c, c]

    def span(q):
        return pl.ds(128 * q, 128)

    ow = [remote(wt.at[span(q), :], wo.at[span(q), mine], to_core) for q in range(2)]
    pieces = [(n, q) for n in range(2) for q in range(2)]
    ux = [remote(part.at[far + order[n], span(q), :], urecv.at[0, order[n], span(q), :], to_x) for n, q in pieces]
    uy = [remote(part.at[own + order[n], span(q), :], urecv.at[0, order[n], span(q), :], to_y) for n, q in pieces]
    uc = [remote(part.at[far + order[n], span(q), :], urecv.at[1, order[n], span(q), :], to_cross) for n, q in pieces]
    lx = remote(lbuf.at[0], lbuf.at[1], to_y)

    for cp in gx:
        cp.start()
    gp.start()
    ld_ql.wait()
    qlb[r, :, qcol] = lo[...].astype(BF16)
    ld_l = local(l_ref, lo)
    ld_l.start()
    qya.start()
    qx.start()

    ld_qr.wait()

    def to_bf(t, carry):
        span = pl.ds(pl.multiple_of(t * 128, 128), 128)
        qro[span, :] = acc[span, other].astype(BF16)
        qrx[c, span, :] = acc[span, mine].astype(BF16)
        return carry

    lax.fori_loop(0, 8, to_bf, 0)
    qrp.start()
    ld_r = local(r_ref, acc)
    ld_r.start()

    ld_g.wait()
    gp.wait_recv()

    @pl.when(diag)
    def _():
        def cast(t, carry):
            span = pl.ds(pl.multiple_of(t * 64, 64), 64)
            for i in range(2):
                for h in range(2):
                    kbuf[h, i, span, :] = gat[0, own + i, span, pl.ds(1024 * h, 1024)].astype(BF16)
            return carry

        lax.fori_loop(0, 4, cast, 0)
        gb[0].start()

    sm.start()
    sv.start()
    sw.start()

    qrp.wait_recv()

    def inner(load, store):
        lhs = [jnp.concatenate([load(0, h), load(1, h)], 0) for h in range(2)]

        def cols(t, carry):
            span = pl.ds(pl.multiple_of(t * 256, 256), 256)
            value = jnp.dot(lhs[0], qrx[0, :, span], preferred_element_type=F32)
            value += jnp.dot(lhs[1], qrx[1, :, span], preferred_element_type=F32)
            store(span, value)
            return carry

        lax.fori_loop(0, 4, cols, 0)

    def send_part(k):
        def store(span, value):
            part[k // 2, pl.ds(128 * (k % 2), 128), span] = value

        inner(lambda i, h: gat[sel, far + i, rows(k), pl.ds(1024 * h, 1024)].astype(BF16), store)
        px[k].start()

    def relay(k):
        @pl.when(off)
        def _():
            y2[k].wait_recv()
            f2[k].start()
            y3[k].wait_recv()
            f3[k].start()
            f2[k].wait_recv()
            f3[k].wait_recv()

    for k in range(CHUNKS):
        gx[k].wait_recv()
        gf[k].start()

        @pl.when(diag)
        def _():
            y2[k].start()

        gf[k].wait_recv()

        @pl.when(diag)
        def _():
            y3[k].start()

        if k == CHUNKS - 1:

            @pl.when(diag)
            def _():
                for n in range(1, CHUNKS):
                    gb[n].start()

        if k > 0:
            relay(k - 1)
            send_part(k - 1)

    qx.wait_recv()
    qyb.start()

    @pl.when(diag)
    def _():
        ya.start()

    relay(CHUNKS - 1)
    send_part(CHUNKS - 1)

    def stat_right(base, t, last):
        lane = pl.ds(pl.multiple_of(c * 1024 + t * 256, 256), 256)
        tall = jnp.concatenate([gat[sel, base, :, lane], gat[sel, base + 1, :, lane]], 0).T
        span = pl.ds(pl.multiple_of(t * 256, 256), 256)

        def cols(n, carry):
            at = pl.ds(pl.multiple_of(n * 256, 256), 256)
            wide = jnp.concatenate([gat[0, base, :, at], gat[0, base + 1, :, at]], 0)
            value = jnp.dot(tall, wide, precision=lax.Precision.HIGHEST, preferred_element_type=F32)
            prev = acc[span, at]
            if not last:
                prev = BETA2 * prev
            acc[span, at] = prev + (1.0 - BETA2) * value
            return carry

        lax.fori_loop(0, 8, cols, 0)

    def gram(k):
        for i in range(2):
            def deep(t, value, i=i):
                lane = pl.ds(pl.multiple_of(t * 256, 256), 256)
                return value + lax.dot_general(
                    gat[0, r, :, lane], gat[0, 2 * k + i, :, lane], nt, precision=lax.Precision.HIGHEST, preferred_element_type=F32
                )

            yield pl.ds(256 * i, 256), lax.fori_loop(0, 8, deep, jnp.zeros((256, 256), F32))

    ld_r.wait()
    ld_l.wait()

    def own_part(k):
        def store(span, value):
            part[2 + k // 2, pl.ds(128 * (k % 2), 128), span] = value

        inner(lambda i, h: kbuf[h, i, rows(k), :], store)

    for k in range(CHUNKS):

        @pl.when(off)
        def _():
            gb[k].wait_recv()
            fb[k].start()
            fb[k].wait_recv()

        own_part(k)
        px[k].wait_recv()
        for i in range(2):
            at = pl.ds(128 * (k % 2) + 64 * i, 64)
            hbuf[own + i, rows(k), :] = (part[2 + k // 2, at, :] + precv[k, pl.ds(64 * i, 64), :]).astype(BF16)
        hx[k].start()
        if k < 3:
            stat_right(far, k, False)

    qya.wait_recv()
    qyb.wait_recv()

    @pl.when(diag)
    def _():
        for cp in gb:
            cp.wait_send()

    @pl.when(off)
    def _():
        for cp in fb:
            cp.wait_send()

    qpa.start()
    qpb.start()
    qpa.wait_recv()
    qpb.wait_recv()

    def turn(t, carry):
        lane = pl.ds(pl.multiple_of(x * 512 + t * 128, 128), 128)
        for p in range(4):
            qlt[pl.ds(pl.multiple_of(t * 128, 128), 128), pl.ds(256 * p, 256)] = qlb[p, :, lane].astype(F32).T.astype(BF16)
        return carry

    lax.fori_loop(0, 4, turn, 0)

    def basis_dot(t, base, at):
        value = jnp.zeros((128, at.size), F32)
        for i in range(2):
            lane = pl.ds(pl.multiple_of((base + i) * 256, 256), 256)
            value += jnp.dot(qlt[pl.ds(pl.multiple_of(t * 128, 128), 128), lane], hbuf[base + i, :, at], preferred_element_type=F32)
        return value

    def own_half(t, carry):
        for h in range(2):
            at = pl.ds(512 * h, 512)
            precv[t, :, at] = basis_dot(t, own, at)
        return carry

    lax.fori_loop(0, 4, own_half, 0)
    stat_right(far, 3, False)
    for at, value in gram(1 - y):
        lbuf[0, :, at] = value
    lx.start()
    ld_m.wait()
    ld_v.wait()
    ld_w.wait()
    sm.wait_recv()
    sv.wait_recv()
    sw.wait_recv()
    for k in range(CHUNKS):
        hx[k].wait_recv()

    for j in range(CHUNKS):
        at = pl.ds(256 * j, 256)
        lane = pl.ds(pl.multiple_of(c * 1024 + 256 * j, 256), 256)
        for n in range(2):
            i = order[n]
            mom, var, cols = (mt, vt, at) if n == 0 else (mo, vo, lane)
            for q in range(2):
                rot = precv[2 * i + q, :, at] + basis_dot(2 * i + q, far, at)
                first = BETA1 * mom[span(q), cols] + (1.0 - BETA1) * rot
                second = BETA2 * var[span(q), cols] + (1.0 - BETA2) * rot * rot
                mom[span(q), cols] = first
                var[span(q), cols] = second
                step = (first / BIAS_ONE) / (jnp.sqrt(second / BIAS_TWO) + EPS)
                nbuf[j, pl.ds(pl.multiple_of(x * 512 + 256 * i + 128 * q, 128), 128), :] = step.astype(BF16)
        nx[j].start()

    om.start()
    ov.start()

    def back(j):
        at = pl.ds(256 * j, 256)
        nx[j].wait_recv()

        for n in range(2):
            two = pl.ds(2 * n, 2)
            value = jnp.dot(qlb[two].reshape(512, 1024), nbuf[j], preferred_element_type=F32)
            kbuf[c, two, :, at] = value.astype(BF16).reshape(2, 256, 256)
        kp[j].start()

    def update(lo, width, first):
        at = pl.ds(lo, width)

        def cols(n, carry):
            lane, two = pl.ds(pl.multiple_of(n // 2 * 256, 256), 256), pl.ds(n % 2 * 2, 2)
            value = lax.dot_general(kbuf[c, two, :, at].reshape(512, width), qrx[c, lane, at], nt, preferred_element_type=F32)
            value += lax.dot_general(kbuf[1 - c, two, :, at].reshape(512, width), qro[lane, at], nt, preferred_element_type=F32)
            value = value.reshape(2, 256, 256)
            part[two, :, lane] = value if first else part[two, :, lane] + value
            return carry

        lax.fori_loop(0, 8, cols, 0)

    last = pl.ds(768, 256)

    def update_mine(n, carry):
        lane, two = pl.ds(pl.multiple_of(n // 2 * 256, 256), 256), pl.ds(n % 2 * 2, 2)
        value = lax.dot_general(kbuf[c, two, :, last].reshape(512, 256), qrx[c, lane, last], nt, preferred_element_type=F32)
        part[two, :, lane] += value.reshape(2, 256, 256)
        return carry

    def update_other(p, q):
        for t in range(4):
            lane = pl.ds(256 * t, 256)
            part[p, span(q), lane] += lax.dot_general(
                kbuf[1 - c, p, span(q), last], qro[lane, last], nt, preferred_element_type=F32
            )

    for k in range(CHUNKS):
        px[k].wait_send()
    back(0)
    back(1)
    kp[0].wait_recv()
    kp[1].wait_recv()
    update(0, 512, True)
    back(2)
    kp[2].wait_recv()
    update(512, 256, False)
    back(3)
    lax.fori_loop(0, 8, update_mine, 0)
    kp[3].wait_recv()
    for n, (m, q) in enumerate(pieces):
        update_other(far + order[m], q)

        @pl.when(diag)
        def _():
            ux[n].start()

        @pl.when(off)
        def _():
            uc[n].start()

        update_other(own + order[m], q)

        @pl.when(off)
        def _():
            uy[n].start()

    @pl.when(off)
    def _():
        ya.wait_recv()

    for t in range(4):
        stat_right(own, t, True)
    for at, value in gram(y):
        lo[:, at] = BETA2 * lo[:, at] + (1.0 - BETA2) * value
    lx.wait_recv()
    lo[...] = lo[...] + (1.0 - BETA2) * lbuf[1]

    for n, (m, q) in enumerate(pieces):
        i = order[m]
        out, cols = (wt, slice(None)) if m == 0 else (wo, mine)

        @pl.when(diag)
        def _():
            uy[n].wait_recv()
            out[span(q), cols] = out[span(q), cols] - LR * (part[own + i, span(q), :] + urecv[0, i, span(q), :])

        @pl.when(off)
        def _():
            ux[n].wait_recv()
            uc[n].wait_recv()
            out[span(q), cols] = out[span(q), cols] - LR * (urecv[0, i, span(q), :] + urecv[1, i, span(q), :])

        if m == 0:
            ow[q].start()

    for cp in [*gx, gp, sm, sv, sw, qx, qya, qyb, qpa, qpb, qrp, *gf, *hx, *nx, *kp, lx]:
        cp.wait_send()

    @pl.when(diag)
    def _():
        for cp in [*y2, *y3, ya, *ux]:
            cp.wait_send()

    @pl.when(off)
    def _():
        for cp in [*f2, *f3, *uy, *uc]:
            cp.wait_send()

    for cp in (om, ov, *ow):
        cp.wait()


def solution(mesh):
    tile_spec = P(("layer", "row"), "col")

    def local_step(weight, grad_in, mom_first, mom_second, stat_left, stat_right, basis_left, basis_right):
        like = lambda a: pltpu.VMEM(a.shape, a.dtype)
        return pl.pallas_call(
            _step,
            out_shape=(like(weight), like(mom_first), like(mom_second), like(stat_left), like(stat_right)),
            in_specs=[pl.BlockSpec(memory_space=pl.ANY)] * 8,
            out_specs=(pl.BlockSpec(memory_space=pltpu.VMEM),) * 5,
            scratch_shapes=[
                pltpu.VMEM((2, 4, 256, 2048), F32),
                pltpu.VMEM((2, 1024, 1024), BF16),
                pltpu.VMEM((1024, 1024), BF16),
                pltpu.VMEM((4, 256, 1024), F32),
                pltpu.VMEM((4, 128, 1024), F32),
                pltpu.VMEM((4, 256, 1024), BF16),
                pltpu.VMEM((4, 256, 1024), BF16),
                pltpu.VMEM((512, 1024), BF16),
                pltpu.VMEM((256, 1024), F32),
                pltpu.VMEM((256, 1024), F32),
                pltpu.VMEM((256, 1024), F32),
                pltpu.VMEM((4, 1024, 256), BF16),
                pltpu.VMEM((2, 4, 256, 1024), BF16),
                pltpu.VMEM((2, 2, 256, 1024), F32),
                pltpu.VMEM((2, 256, 512), F32),
                pltpu.SemaphoreType.DMA((COPIES,)),
                pltpu.SemaphoreType.DMA((COPIES,)),
                pltpu.SemaphoreType.DMA((24,)),
            ],
            compiler_params=pltpu.CompilerParams(collective_id=0, has_side_effects=True, vmem_limit_bytes=GRANT),
        )(weight, grad_in, mom_first, mom_second, stat_left, stat_right, basis_left, basis_right)

    return jax.shard_map(local_step, mesh=mesh, in_specs=(tile_spec,) * 8, out_specs=(tile_spec,) * 5, check_vma=False)
```

```python
import functools

import jax
import jax.numpy as jnp
from jax import lax
from jax.experimental import pallas as pl
from jax.experimental.pallas import tpu as pltpu
from jax.sharding import PartitionSpec as P

BETA1 = 0.9
BETA2 = 0.9
EPS = 1e-8
LR = 0.1
STEP = 10
BIAS_ONE = 1.0 - BETA1 ** STEP
BIAS_TWO = 1.0 - BETA2 ** STEP

MESH = pl.DeviceIdType.MESH
F32, BF16 = jnp.float32, jnp.bfloat16
CHUNKS = 4
COPIES = 84
GRANT = 51800000


def _step(
    w_ref, g_ref, m_ref, v_ref, l_ref, r_ref, ql_ref, qr_ref,
    wo, mo, vo, lo, acc,
    gat, qrx, qro, part, precv, hbuf, qlb, qlt, mt, vt, wt, nbuf, kbuf, urecv, lbuf,
    ssem, rsem, lsem,
):
    y, r = lax.axis_index("col"), lax.axis_index("row")
    x, c = r // 2, r % 2
    diag = x == y
    off = x != y
    sel = jnp.where(diag, 0, 1)
    own, far = 2 * x, 2 * (1 - x)
    rx = 2 * (1 - x) + c
    rp = 2 * x + 1 - c
    rxp = 2 * (1 - x) + 1 - c
    mine = pl.ds(pl.multiple_of(c * 1024, 1024), 1024)
    other = pl.ds(pl.multiple_of((1 - c) * 1024, 1024), 1024)
    to_x, to_core, to_y, to_cross = (0, y, rx), (0, y, rp), (0, 1 - y, r), (0, 1 - y, rx)

    nt = (((1,), (1,)), ((), ()))
    used = [0]
    local_used = [0]

    def remote(src, dst, dev):
        n = used[0]
        used[0] += 1
        return pltpu.make_async_remote_copy(
            src_ref=src, dst_ref=dst, send_sem=ssem.at[n], recv_sem=rsem.at[n], device_id=dev, device_id_type=MESH
        )

    def local(src, dst):
        n = local_used[0]
        local_used[0] += 1
        return pltpu.make_async_copy(src, dst, lsem.at[n])

    ld_g = local(g_ref, gat.at[0, r])
    ld_qr = local(qr_ref, acc)
    ld_ql = local(ql_ref, lo)
    ld_m = local(m_ref.at[:, mine], mo.at[:, mine])
    ld_v = local(v_ref.at[:, mine], vo.at[:, mine])
    ld_w = local(w_ref.at[:, mine], wo.at[:, mine])
    for cp in (ld_ql, ld_qr, ld_g, ld_m, ld_v, ld_w):
        cp.start()

    barrier = pltpu.get_barrier_semaphore()
    for dev in (to_x, to_core, to_y, to_cross):
        pl.semaphore_signal(barrier, inc=1, device_id=dev, device_id_type=MESH)
    pl.semaphore_wait(barrier, 4)

    def rows(k):
        return pl.ds(64 * k, 64)

    gx = [remote(g_ref.at[rows(k), :], gat.at[0, r, rows(k), :], to_x) for k in range(CHUNKS)]
    gp = remote(g_ref, gat.at[0, r], to_core)
    sm = remote(m_ref.at[:, other], mt, to_core)
    sv = remote(v_ref.at[:, other], vt, to_core)
    sw = remote(w_ref.at[:, other], wt, to_core)
    qcol = pl.ds(pl.multiple_of(y * 512, 512), 512)
    qx = remote(qlb.at[r, :, qcol], qlb.at[r, :, qcol], to_x)
    qya = remote(qlb.at[r, :, qcol], qlb.at[r, :, qcol], to_y)
    qyb = remote(qlb.at[rx, :, qcol], qlb.at[rx, :, qcol], to_y)
    qpa = remote(qlb.at[r], qlb.at[r], to_core)
    qpb = remote(qlb.at[rx], qlb.at[rx], to_core)
    qrp = remote(qro, qrx.at[c], to_core)
    gb = [remote(kbuf.at[c, pl.ds(0, 2), rows(k), :], kbuf.at[c, pl.ds(0, 2), rows(k), :], to_y) for k in range(CHUNKS)]
    fb = [remote(kbuf.at[c, pl.ds(0, 2), rows(k), :], kbuf.at[c, pl.ds(0, 2), rows(k), :], to_core) for k in range(CHUNKS)]
    gf = [remote(gat.at[0, rx, rows(k), :], gat.at[0, rx, rows(k), :], to_core) for k in range(CHUNKS)]
    y2 = [remote(gat.at[0, rx, rows(k), mine], gat.at[1, rx, rows(k), mine], to_y) for k in range(CHUNKS)]
    y3 = [remote(gat.at[0, rxp, rows(k), mine], gat.at[1, rxp, rows(k), mine], to_y) for k in range(CHUNKS)]
    f2 = [remote(gat.at[1, rx, rows(k), mine], gat.at[1, rx, rows(k), mine], to_core) for k in range(CHUNKS)]
    f3 = [remote(gat.at[1, rxp, rows(k), mine], gat.at[1, rxp, rows(k), mine], to_core) for k in range(CHUNKS)]
    ya = remote(gat.at[0, pl.ds(own, 2), :, mine], gat.at[1, pl.ds(own, 2), :, mine], to_y)

    def pslot(base, k):
        return part.at[base + k // 2, pl.ds(128 * (k % 2), 128), :]

    px = [remote(pslot(0, k), precv.at[k], to_x) for k in range(CHUNKS)]
    hx = [remote(hbuf.at[pl.ds(own, 2), rows(k), :], hbuf.at[pl.ds(own, 2), rows(k), :], to_x) for k in range(CHUNKS - 1)]
    tail = [(pl.ds(own, 2), rows(CHUNKS - 1), pl.ds(256 * j, 256)) for j in range(4)]
    hc = [remote(hbuf.at[t], hbuf.at[t], to_x) for t in tail]
    half = pl.ds(pl.multiple_of(x * 512, 512), 512)
    nx = [remote(nbuf.at[j, half, :], nbuf.at[j, half, :], to_x) for j in range(CHUNKS)]
    kcut = [(c, pl.ds(base, 2), slice(None), pl.ds(256 * j, 256)) for j in range(CHUNKS) for base in (far, own)]
    kp = [remote(kbuf.at[cut], kbuf.at[cut], to_core) for cut in kcut]
    om = remote(mt, mo.at[:, mine], to_core)
    ov = remote(vt, vo.at[:, mine], to_core)
    order = [1 - c, c]

    def span(q):
        return pl.ds(128 * q, 128)

    ow = [remote(wt.at[span(q), :], wo.at[span(q), mine], to_core) for q in range(2)]
    pieces = [(n, q) for n in range(2) for q in range(2)]
    ux = [remote(part.at[far + order[n], span(q), :], urecv.at[0, order[n], span(q), :], to_x) for n, q in pieces]
    uy = [remote(part.at[own + order[n], span(q), :], urecv.at[0, order[n], span(q), :], to_y) for n, q in pieces]
    uc = [remote(part.at[far + order[n], span(q), :], urecv.at[1, order[n], span(q), :], to_cross) for n, q in pieces]
    lx = remote(lbuf.at[0], lbuf.at[1], to_y)

    for cp in gx:
        cp.start()
    gp.start()
    ld_ql.wait()
    qlb[r, :, qcol] = lo[...].astype(BF16)
    ld_l = local(l_ref, lo)
    ld_l.start()
    qya.start()
    qx.start()

    ld_qr.wait()

    def to_bf(t, carry):
        span = pl.ds(pl.multiple_of(t * 128, 128), 128)
        qro[span, :] = acc[span, other].astype(BF16)
        qrx[c, span, :] = acc[span, mine].astype(BF16)
        return carry

    lax.fori_loop(0, 8, to_bf, 0)
    qrp.start()
    ld_r = local(r_ref, acc)
    ld_r.start()

    ld_g.wait()
    gp.wait_recv()

    @pl.when(diag)
    def _():
        def cast(t, carry):
            span = pl.ds(pl.multiple_of(t * 64, 64), 64)
            for i in range(2):
                for h in range(2):
                    kbuf[h, i, span, :] = gat[0, own + i, span, pl.ds(1024 * h, 1024)].astype(BF16)
            return carry

        lax.fori_loop(0, 4, cast, 0)
        gb[0].start()

    sm.start()
    sv.start()
    sw.start()

    qrp.wait_recv()

    def inner(load, store):
        lhs = [jnp.concatenate([load(0, h), load(1, h)], 0) for h in range(2)]

        def cols(t, carry):
            span = pl.ds(pl.multiple_of(t * 256, 256), 256)
            value = jnp.dot(lhs[0], qrx[0, :, span], preferred_element_type=F32)
            value += jnp.dot(lhs[1], qrx[1, :, span], preferred_element_type=F32)
            store(span, value)
            return carry

        lax.fori_loop(0, 4, cols, 0)

    def send_part(k):
        def store(span, value):
            part[k // 2, pl.ds(128 * (k % 2), 128), span] = value

        inner(lambda i, h: gat[sel, far + i, rows(k), pl.ds(1024 * h, 1024)].astype(BF16), store)
        px[k].start()

    def relay(k):
        @pl.when(off)
        def _():
            y2[k].wait_recv()
            f2[k].start()
            y3[k].wait_recv()
            f3[k].start()
            f2[k].wait_recv()
            f3[k].wait_recv()

    for k in range(CHUNKS):
        gx[k].wait_recv()
        gf[k].start()

        @pl.when(diag)
        def _():
            y2[k].start()

        gf[k].wait_recv()

        @pl.when(diag)
        def _():
            y3[k].start()

        if k == CHUNKS - 1:

            @pl.when(diag)
            def _():
                for n in range(1, CHUNKS):
                    gb[n].start()

        if k > 0:
            relay(k - 1)
            send_part(k - 1)

    qx.wait_recv()
    qyb.start()

    @pl.when(diag)
    def _():
        ya.start()

    relay(CHUNKS - 1)
    send_part(CHUNKS - 1)

    def stat_right(base, t, last):
        lane = pl.ds(pl.multiple_of(c * 1024 + t * 256, 256), 256)
        tall = jnp.concatenate([gat[sel, base, :, lane], gat[sel, base + 1, :, lane]], 0).T
        span = pl.ds(pl.multiple_of(t * 256, 256), 256)

        def cols(n, carry):
            at = pl.ds(pl.multiple_of(n * 256, 256), 256)
            wide = jnp.concatenate([gat[0, base, :, at], gat[0, base + 1, :, at]], 0)
            value = jnp.dot(tall, wide, precision=lax.Precision.HIGHEST, preferred_element_type=F32)
            prev = acc[span, at]
            if not last:
                prev = BETA2 * prev
            acc[span, at] = prev + (1.0 - BETA2) * value
            return carry

        lax.fori_loop(0, 8, cols, 0)

    def gram(k):
        for i in range(2):
            def deep(t, value, i=i):
                lane = pl.ds(pl.multiple_of(t * 256, 256), 256)
                return value + lax.dot_general(
                    gat[0, r, :, lane], gat[0, 2 * k + i, :, lane], nt, precision=lax.Precision.HIGHEST, preferred_element_type=F32
                )

            yield pl.ds(256 * i, 256), lax.fori_loop(0, 8, deep, jnp.zeros((256, 256), F32))

    ld_r.wait()
    ld_l.wait()

    def own_part(k):
        def store(span, value):
            part[2 + k // 2, pl.ds(128 * (k % 2), 128), span] = value

        inner(lambda i, h: kbuf[h, i, rows(k), :], store)

    for k in range(CHUNKS):

        @pl.when(off)
        def _():
            gb[k].wait_recv()
            fb[k].start()
            fb[k].wait_recv()

        own_part(k)
        px[k].wait_recv()
        for i in range(2):
            at = pl.ds(128 * (k % 2) + 64 * i, 64)
            hbuf[own + i, rows(k), :] = (part[2 + k // 2, at, :] + precv[k, pl.ds(64 * i, 64), :]).astype(BF16)
        if k < CHUNKS - 1:
            hx[k].start()
            stat_right(far, k, False)
    for cp in hc:
        cp.start()

    qya.wait_recv()
    qyb.wait_recv()

    @pl.when(diag)
    def _():
        for cp in gb:
            cp.wait_send()

    @pl.when(off)
    def _():
        for cp in fb:
            cp.wait_send()

    qpa.start()
    qpb.start()
    qpa.wait_recv()
    qpb.wait_recv()

    def turn(t, carry):
        lane = pl.ds(pl.multiple_of(x * 512 + t * 128, 128), 128)
        for p in range(4):
            qlt[pl.ds(pl.multiple_of(t * 128, 128), 128), pl.ds(256 * p, 256)] = qlb[p, :, lane].astype(F32).T.astype(BF16)
        return carry

    lax.fori_loop(0, 4, turn, 0)

    def basis_dot(t, base, at):
        value = jnp.zeros((128, at.size), F32)
        for i in range(2):
            lane = pl.ds(pl.multiple_of((base + i) * 256, 256), 256)
            value += jnp.dot(qlt[pl.ds(pl.multiple_of(t * 128, 128), 128), lane], hbuf[base + i, :, at], preferred_element_type=F32)
        return value

    def own_half(t, carry):
        for h in range(2):
            at = pl.ds(512 * h, 512)
            precv[t, :, at] = basis_dot(t, own, at)
        return carry

    lax.fori_loop(0, 4, own_half, 0)
    stat_right(far, 3, False)
    for at, value in gram(1 - y):
        lbuf[0, :, at] = value
    lx.start()
    ld_m.wait()
    ld_v.wait()
    ld_w.wait()
    sm.wait_recv()
    sv.wait_recv()
    sw.wait_recv()
    for cp in hx:
        cp.wait_recv()

    for j in range(CHUNKS):
        hc[j].wait_recv()
        at = pl.ds(256 * j, 256)
        lane = pl.ds(pl.multiple_of(c * 1024 + 256 * j, 256), 256)
        for n in range(2):
            i = order[n]
            mom, var, cols = (mt, vt, at) if n == 0 else (mo, vo, lane)
            for q in range(2):
                rot = precv[2 * i + q, :, at] + basis_dot(2 * i + q, far, at)
                first = BETA1 * mom[span(q), cols] + (1.0 - BETA1) * rot
                second = BETA2 * var[span(q), cols] + (1.0 - BETA2) * rot * rot
                mom[span(q), cols] = first
                var[span(q), cols] = second
                step = (first / BIAS_ONE) / (jnp.sqrt(second / BIAS_TWO) + EPS)
                nbuf[j, pl.ds(pl.multiple_of(x * 512 + 256 * i + 128 * q, 128), 128), :] = step.astype(BF16)
        nx[j].start()

    om.start()
    ov.start()

    def back(j):
        at = pl.ds(256 * j, 256)
        nx[j].wait_recv()
        for n, base in enumerate((far, own)):
            two = pl.ds(base, 2)
            value = jnp.dot(qlb[two].reshape(512, 1024), nbuf[j], preferred_element_type=F32)
            kbuf[c, two, :, at] = value.astype(BF16).reshape(2, 256, 256)
            kp[2 * j + n].start()

    def update(lo, width, first):
        at = pl.ds(lo, width)

        def cols(n, carry):
            lane, two = pl.ds(pl.multiple_of(n // 2 * 256, 256), 256), pl.ds(n % 2 * 2, 2)
            value = lax.dot_general(kbuf[c, two, :, at].reshape(512, width), qrx[c, lane, at], nt, preferred_element_type=F32)
            value += lax.dot_general(kbuf[1 - c, two, :, at].reshape(512, width), qro[lane, at], nt, preferred_element_type=F32)
            value = value.reshape(2, 256, 256)
            part[two, :, lane] = value if first else part[two, :, lane] + value
            return carry

        lax.fori_loop(0, 8, cols, 0)

    last = pl.ds(768, 256)

    def update_mine(n, carry):
        lane, two = pl.ds(pl.multiple_of(n // 2 * 256, 256), 256), pl.ds(n % 2 * 2, 2)
        value = lax.dot_general(kbuf[c, two, :, last].reshape(512, 256), qrx[c, lane, last], nt, preferred_element_type=F32)
        part[two, :, lane] += value.reshape(2, 256, 256)
        return carry

    def update_other(p, q):
        for t in range(4):
            lane = pl.ds(256 * t, 256)
            part[p, span(q), lane] += lax.dot_general(
                kbuf[1 - c, p, span(q), last], qro[lane, last], nt, preferred_element_type=F32
            )

    for k in range(CHUNKS):
        px[k].wait_send()
    back(0)
    back(1)
    for cp in kp[:4]:
        cp.wait_recv()
    update(0, 512, True)
    back(2)
    for cp in kp[4:6]:
        cp.wait_recv()
    update(512, 256, False)
    back(3)
    lax.fori_loop(0, 8, update_mine, 0)
    kp[6].wait_recv()
    for n, (m, q) in enumerate(pieces):
        update_other(far + order[m], q)

        @pl.when(diag)
        def _():
            ux[n].start()

        @pl.when(off)
        def _():
            uc[n].start()

        if n == 0:
            kp[7].wait_recv()
        update_other(own + order[m], q)

        @pl.when(off)
        def _():
            uy[n].start()

    @pl.when(off)
    def _():
        ya.wait_recv()

    for t in range(4):
        stat_right(own, t, True)
    for at, value in gram(y):
        lo[:, at] = BETA2 * lo[:, at] + (1.0 - BETA2) * value
    lx.wait_recv()
    lo[...] = lo[...] + (1.0 - BETA2) * lbuf[1]

    for n, (m, q) in enumerate(pieces):
        i = order[m]
        out, cols = (wt, slice(None)) if m == 0 else (wo, mine)

        @pl.when(diag)
        def _():
            uy[n].wait_recv()
            out[span(q), cols] = out[span(q), cols] - LR * (part[own + i, span(q), :] + urecv[0, i, span(q), :])

        @pl.when(off)
        def _():
            ux[n].wait_recv()
            uc[n].wait_recv()
            out[span(q), cols] = out[span(q), cols] - LR * (urecv[0, i, span(q), :] + urecv[1, i, span(q), :])

        if m == 0:
            ow[q].start()

    for cp in [*gx, gp, sm, sv, sw, qx, qya, qyb, qpa, qpb, qrp, *gf, *hx, *hc, *nx, *kp, lx]:
        cp.wait_send()

    @pl.when(diag)
    def _():
        for cp in [*y2, *y3, ya, *ux]:
            cp.wait_send()

    @pl.when(off)
    def _():
        for cp in [*f2, *f3, *uy, *uc]:
            cp.wait_send()

    for cp in (om, ov, *ow):
        cp.wait()


def _write(*refs):
    sems = refs[-1]
    count = (len(refs) - 1) // 2
    copies = [pltpu.make_async_copy(refs[n], refs[count + n], sems.at[n]) for n in range(count)]
    for cp in copies:
        cp.start()
    for cp in copies:
        cp.wait()


def solution(mesh):
    tile_spec = P(("layer", "row"), "col")

    def local_step(weight, grad_in, mom_first, mom_second, stat_left, stat_right, basis_left, basis_right):
        like = lambda a: pltpu.VMEM(a.shape, a.dtype)
        outs = pl.pallas_call(
            _step,
            out_shape=(like(weight), like(mom_first), like(mom_second), like(stat_left), like(stat_right)),
            in_specs=[pl.BlockSpec(memory_space=pl.ANY)] * 8,
            out_specs=(pl.BlockSpec(memory_space=pltpu.VMEM),) * 5,
            scratch_shapes=[
                pltpu.VMEM((2, 4, 256, 2048), F32),
                pltpu.VMEM((2, 1024, 1024), BF16),
                pltpu.VMEM((1024, 1024), BF16),
                pltpu.VMEM((4, 256, 1024), F32),
                pltpu.VMEM((4, 128, 1024), F32),
                pltpu.VMEM((4, 256, 1024), BF16),
                pltpu.VMEM((4, 256, 1024), BF16),
                pltpu.VMEM((512, 1024), BF16),
                pltpu.VMEM((256, 1024), F32),
                pltpu.VMEM((256, 1024), F32),
                pltpu.VMEM((256, 1024), F32),
                pltpu.VMEM((4, 1024, 256), BF16),
                pltpu.VMEM((2, 4, 256, 1024), BF16),
                pltpu.VMEM((2, 2, 256, 1024), F32),
                pltpu.VMEM((2, 256, 512), F32),
                pltpu.SemaphoreType.DMA((COPIES,)),
                pltpu.SemaphoreType.DMA((COPIES,)),
                pltpu.SemaphoreType.DMA((24,)),
            ],
            compiler_params=pltpu.CompilerParams(collective_id=0, has_side_effects=True, vmem_limit_bytes=GRANT),
        )(weight, grad_in, mom_first, mom_second, stat_left, stat_right, basis_left, basis_right)
        return pl.pallas_call(
            _write,
            out_shape=tuple(jax.ShapeDtypeStruct(o.shape, o.dtype) for o in outs),
            in_specs=[pl.BlockSpec(memory_space=pltpu.VMEM)] * 5,
            out_specs=(pl.BlockSpec(memory_space=pl.ANY),) * 5,
            scratch_shapes=[pltpu.SemaphoreType.DMA((5,))],
            compiler_params=pltpu.CompilerParams(vmem_limit_bytes=1048576),
        )(*(pltpu.with_memory_space_constraint(o, pltpu.VMEM) for o in outs))

    return jax.shard_map(local_step, mesh=mesh, in_specs=(tile_spec,) * 8, out_specs=(tile_spec,) * 5, check_vma=False)
```

```python
import functools

import jax
import jax.numpy as jnp
from jax import lax
from jax.experimental import pallas as pl
from jax.experimental.pallas import tpu as pltpu
from jax.sharding import PartitionSpec as P

BETA1 = 0.9
BETA2 = 0.9
EPS = 1e-8
LR = 0.1
STEP = 10
BIAS_ONE = 1.0 - BETA1 ** STEP
BIAS_TWO = 1.0 - BETA2 ** STEP

MESH = pl.DeviceIdType.MESH
F32, BF16 = jnp.float32, jnp.bfloat16
CHUNKS = 4
COPIES = 83
UNROLL = 2
GRANT = 51800000


def _step(
    w_ref, g_ref, m_ref, v_ref, l_ref, r_ref, ql_ref, qr_ref,
    wo, mo, vo, lo, acc,
    gat, qrx, qro, part, precv, hbuf, qlb, qlt, mt, vt, wt, nbuf, kbuf, urecv, lbuf,
    ssem, rsem, lsem,
):
    y, r = lax.axis_index("col"), lax.axis_index("row")
    x, c = r // 2, r % 2
    diag = x == y
    off = x != y
    sel = jnp.where(diag, 0, 1)
    own, far = 2 * x, 2 * (1 - x)
    rx = 2 * (1 - x) + c
    rp = 2 * x + 1 - c
    rxp = 2 * (1 - x) + 1 - c
    mine = pl.ds(pl.multiple_of(c * 1024, 1024), 1024)
    other = pl.ds(pl.multiple_of((1 - c) * 1024, 1024), 1024)
    to_x, to_core, to_y, to_cross = (0, y, rx), (0, y, rp), (0, 1 - y, r), (0, 1 - y, rx)

    nt = (((1,), (1,)), ((), ()))
    used = [0]
    local_used = [0]

    def remote(src, dst, dev):
        n = used[0]
        used[0] += 1
        return pltpu.make_async_remote_copy(
            src_ref=src, dst_ref=dst, send_sem=ssem.at[n], recv_sem=rsem.at[n], device_id=dev, device_id_type=MESH
        )

    def local(src, dst):
        n = local_used[0]
        local_used[0] += 1
        return pltpu.make_async_copy(src, dst, lsem.at[n])

    ld_g = local(g_ref, gat.at[0, r])
    ld_qr = local(qr_ref, acc)
    ld_ql = local(ql_ref, lo)
    ld_m = local(m_ref.at[:, mine], mo.at[:, mine])
    ld_v = local(v_ref.at[:, mine], vo.at[:, mine])
    ld_w = local(w_ref.at[:, mine], wo.at[:, mine])
    for cp in (ld_ql, ld_qr, ld_g, ld_m, ld_v, ld_w):
        cp.start()

    barrier = pltpu.get_barrier_semaphore()
    for dev in (to_x, to_core, to_y, to_cross):
        pl.semaphore_signal(barrier, inc=1, device_id=dev, device_id_type=MESH)
    pl.semaphore_wait(barrier, 4)

    def rows(k):
        return pl.ds(64 * k, 64)

    gx = [remote(g_ref.at[rows(k), :], gat.at[0, r, rows(k), :], to_x) for k in range(CHUNKS)]
    gp = remote(g_ref, gat.at[0, r], to_core)
    sm = remote(m_ref.at[:, other], mt, to_core)
    sv = remote(v_ref.at[:, other], vt, to_core)
    sw = remote(w_ref.at[:, other], wt, to_core)
    qcol = pl.ds(pl.multiple_of(y * 512, 512), 512)
    qx = remote(qlb.at[r, :, qcol], qlb.at[r, :, qcol], to_x)
    qya = remote(qlb.at[r, :, qcol], qlb.at[r, :, qcol], to_y)
    qyb = remote(qlb.at[rx, :, qcol], qlb.at[rx, :, qcol], to_y)
    qpa = remote(qlb.at[r], qlb.at[r], to_core)
    qpb = remote(qlb.at[rx], qlb.at[rx], to_core)
    qrp = remote(qro, qrx.at[c], to_core)
    gb = [remote(kbuf.at[c, pl.ds(0, 2), rows(k), :], kbuf.at[c, pl.ds(0, 2), rows(k), :], to_y) for k in range(CHUNKS)]
    fb = [remote(kbuf.at[c, pl.ds(0, 2), rows(k), :], kbuf.at[c, pl.ds(0, 2), rows(k), :], to_core) for k in range(CHUNKS)]
    gf = [remote(gat.at[0, rx, rows(k), :], gat.at[0, rx, rows(k), :], to_core) for k in range(CHUNKS)]
    y2 = [remote(gat.at[0, rx, rows(k), mine], gat.at[1, rx, rows(k), mine], to_y) for k in range(CHUNKS)]
    y3 = [remote(gat.at[0, rxp, rows(k), mine], gat.at[1, rxp, rows(k), mine], to_y) for k in range(CHUNKS)]
    f2 = [remote(gat.at[1, rx, rows(k), mine], gat.at[1, rx, rows(k), mine], to_core) for k in range(CHUNKS)]
    f3 = [remote(gat.at[1, rxp, rows(k), mine], gat.at[1, rxp, rows(k), mine], to_core) for k in range(CHUNKS)]
    ya = remote(gat.at[0, pl.ds(own, 2), :, mine], gat.at[1, pl.ds(own, 2), :, mine], to_y)

    def pslot(base, k):
        return part.at[base + k // 2, pl.ds(128 * (k % 2), 128), :]

    px = [remote(pslot(0, k), precv.at[k], to_x) for k in range(CHUNKS)]
    hx = [remote(hbuf.at[pl.ds(own, 2), rows(k), :], hbuf.at[pl.ds(own, 2), rows(k), :], to_x) for k in range(CHUNKS - 1)]
    tail = [(pl.ds(own, 2), rows(CHUNKS - 1), pl.ds(256 * j, 256)) for j in range(4)]
    hc = [remote(hbuf.at[t], hbuf.at[t], to_x) for t in tail]
    half = pl.ds(pl.multiple_of(x * 512, 512), 512)
    nx = [remote(nbuf.at[j, half, :], nbuf.at[j, half, :], to_x) for j in range(CHUNKS)]
    kcut = [(c, pl.ds(base, 2), slice(None), pl.ds(256 * j, 256)) for j in range(CHUNKS) for base in (far, own)]
    kp = [remote(kbuf.at[cut], kbuf.at[cut], to_core) for cut in kcut]
    om = remote(mt, mo.at[:, mine], to_core)
    ov = remote(vt, vo.at[:, mine], to_core)
    order = [1 - c, c]

    def span(q):
        return pl.ds(128 * q, 128)

    ow = [remote(wt.at[span(q), :], wo.at[span(q), mine], to_core) for q in range(2)]
    pieces = [(n, q) for n in range(2) for q in range(2)]
    ux = [remote(part.at[far + order[n], span(q), :], urecv.at[0, order[n], span(q), :], to_x) for n, q in pieces]
    uy = [remote(part.at[own + order[n], span(q), :], urecv.at[0, order[n], span(q), :], to_y) for n, q in pieces]
    uc = [remote(part.at[far + order[n], span(q), :], urecv.at[1, order[n], span(q), :], to_cross) for n, q in pieces]
    lx = remote(lbuf.at[0], lbuf.at[1], to_y)

    for cp in gx:
        cp.start()
    gp.start()
    ld_ql.wait()
    qlb[r, :, qcol] = lo[...].astype(BF16)
    ld_l = local(l_ref, lo)
    ld_l.start()
    qya.start()
    qx.start()

    ld_qr.wait()

    def to_bf(t, carry):
        span = pl.ds(pl.multiple_of(t * 128, 128), 128)
        qro[span, :] = acc[span, other].astype(BF16)
        qrx[c, span, :] = acc[span, mine].astype(BF16)
        return carry

    lax.fori_loop(0, 8, to_bf, 0)
    qrp.start()
    ld_r = local(r_ref, acc)
    ld_r.start()

    ld_g.wait()
    gp.wait_recv()

    @pl.when(diag)
    def _():
        def cast(t, carry):
            span = pl.ds(pl.multiple_of(t * 64, 64), 64)
            for i in range(2):
                for h in range(2):
                    kbuf[h, i, span, :] = gat[0, own + i, span, pl.ds(1024 * h, 1024)].astype(BF16)
            return carry

        lax.fori_loop(0, 4, cast, 0)
        gb[0].start()

    sm.start()
    sv.start()
    sw.start()

    qrp.wait_recv()

    def inner(load, store):
        lhs = [jnp.concatenate([load(0, h), load(1, h)], 0) for h in range(2)]

        def cols(t, carry):
            span = pl.ds(pl.multiple_of(t * 256, 256), 256)
            value = jnp.dot(lhs[0], qrx[0, :, span], preferred_element_type=F32)
            value += jnp.dot(lhs[1], qrx[1, :, span], preferred_element_type=F32)
            store(span, value)
            return carry

        lax.fori_loop(0, 4, cols, 0)

    def send_part(k):
        def store(span, value):
            part[k // 2, pl.ds(128 * (k % 2), 128), span] = value

        inner(lambda i, h: gat[sel, far + i, rows(k), pl.ds(1024 * h, 1024)].astype(BF16), store)
        px[k].start()

    def relay(k):
        @pl.when(off)
        def _():
            y2[k].wait_recv()
            f2[k].start()
            y3[k].wait_recv()
            f3[k].start()
            f2[k].wait_recv()
            f3[k].wait_recv()

    for k in range(CHUNKS):
        gx[k].wait_recv()
        gf[k].start()

        @pl.when(diag)
        def _():
            y2[k].start()

        gf[k].wait_recv()

        @pl.when(diag)
        def _():
            y3[k].start()

        if k == CHUNKS - 1:

            @pl.when(diag)
            def _():
                for n in range(1, CHUNKS):
                    gb[n].start()

        if k > 0:
            relay(k - 1)
            send_part(k - 1)

    qx.wait_recv()
    qyb.start()

    @pl.when(diag)
    def _():
        ya.start()

    relay(CHUNKS - 1)
    send_part(CHUNKS - 1)

    def stat_right(base, t, last):
        lane = pl.ds(pl.multiple_of(c * 1024 + t * 256, 256), 256)
        tall = jnp.concatenate([gat[sel, base, :, lane], gat[sel, base + 1, :, lane]], 0).T
        span = pl.ds(pl.multiple_of(t * 256, 256), 256)

        def cols(n, carry):
            at = pl.ds(pl.multiple_of(n * 256, 256), 256)
            wide = jnp.concatenate([gat[0, base, :, at], gat[0, base + 1, :, at]], 0)
            value = jnp.dot(tall, wide, precision=lax.Precision.HIGHEST, preferred_element_type=F32)
            prev = acc[span, at]
            if not last:
                prev = BETA2 * prev
            acc[span, at] = prev + (1.0 - BETA2) * value
            return carry

        lax.fori_loop(0, 8, cols, 0)

    def gram(k):
        for i in range(2):
            def deep(t, value, i=i):
                lane = pl.ds(pl.multiple_of(t * 256, 256), 256)
                return value + lax.dot_general(
                    gat[0, r, :, lane], gat[0, 2 * k + i, :, lane], nt, precision=lax.Precision.HIGHEST, preferred_element_type=F32
                )

            yield pl.ds(256 * i, 256), lax.fori_loop(0, 8, deep, jnp.zeros((256, 256), F32))

    ld_r.wait()
    ld_l.wait()

    def own_part(k):
        def store(span, value):
            part[2 + k // 2, pl.ds(128 * (k % 2), 128), span] = value

        inner(lambda i, h: kbuf[h, i, rows(k), :], store)

    for k in range(CHUNKS):

        @pl.when(off)
        def _():
            gb[k].wait_recv()
            fb[k].start()
            fb[k].wait_recv()

        own_part(k)
        px[k].wait_recv()
        for i in range(2):
            at = pl.ds(128 * (k % 2) + 64 * i, 64)
            hbuf[own + i, rows(k), :] = (part[2 + k // 2, at, :] + precv[k, pl.ds(64 * i, 64), :]).astype(BF16)
        if k < CHUNKS - 1:
            hx[k].start()
            stat_right(far, k, False)
    for cp in hc:
        cp.start()

    qya.wait_recv()
    qyb.wait_recv()

    @pl.when(diag)
    def _():
        for cp in gb:
            cp.wait_send()

    @pl.when(off)
    def _():
        for cp in fb:
            cp.wait_send()

    qpa.start()
    qpb.start()
    qpa.wait_recv()
    qpb.wait_recv()

    def turn(t, carry):
        lane = pl.ds(pl.multiple_of(x * 512 + t * 128, 128), 128)
        for p in range(4):
            qlt[pl.ds(pl.multiple_of(t * 128, 128), 128), pl.ds(256 * p, 256)] = qlb[p, :, lane].astype(F32).T.astype(BF16)
        return carry

    lax.fori_loop(0, 4, turn, 0)

    def basis_dot(t, base, at):
        value = jnp.zeros((128, at.size), F32)
        for i in range(2):
            lane = pl.ds(pl.multiple_of((base + i) * 256, 256), 256)
            value += jnp.dot(qlt[pl.ds(pl.multiple_of(t * 128, 128), 128), lane], hbuf[base + i, :, at], preferred_element_type=F32)
        return value

    def own_half(t, carry):
        for h in range(2):
            at = pl.ds(512 * h, 512)
            precv[t, :, at] = basis_dot(t, own, at)
        return carry

    lax.fori_loop(0, 4, own_half, 0)
    stat_right(far, 3, False)
    for at, value in gram(1 - y):
        lbuf[0, :, at] = value
    lx.start()
    ld_m.wait()
    ld_v.wait()
    ld_w.wait()
    sm.wait_recv()
    sv.wait_recv()
    sw.wait_recv()
    for cp in hx:
        cp.wait_recv()

    for j in range(CHUNKS):
        hc[j].wait_recv()
        at = pl.ds(256 * j, 256)
        lane = pl.ds(pl.multiple_of(c * 1024 + 256 * j, 256), 256)
        for n in range(2):
            i = order[n]
            mom, var, cols = (mt, vt, at) if n == 0 else (mo, vo, lane)
            for q in range(2):
                rot = precv[2 * i + q, :, at] + basis_dot(2 * i + q, far, at)
                first = BETA1 * mom[span(q), cols] + (1.0 - BETA1) * rot
                second = BETA2 * var[span(q), cols] + (1.0 - BETA2) * rot * rot
                mom[span(q), cols] = first
                var[span(q), cols] = second
                step = (first / BIAS_ONE) / (jnp.sqrt(second / BIAS_TWO) + EPS)
                nbuf[j, pl.ds(pl.multiple_of(x * 512 + 256 * i + 128 * q, 128), 128), :] = step.astype(BF16)
        nx[j].start()

    om.start()
    ov.start()

    def back(j):
        at = pl.ds(256 * j, 256)
        nx[j].wait_recv()
        for n, base in enumerate((far, own)):
            two = pl.ds(base, 2)
            value = jnp.dot(qlb[two].reshape(512, 1024), nbuf[j], preferred_element_type=F32)
            kbuf[c, two, :, at] = value.astype(BF16).reshape(2, 256, 256)
            kp[2 * j + n].start()

    def update(lo, width, near, first=False):
        at = pl.ds(lo, width)
        core, basis = (c, qrx.at[c]) if near else (1 - c, qro)

        def cols(n, carry):
            lane, two = pl.ds(pl.multiple_of(n // 2 * 256, 256), 256), pl.ds(n % 2 * 2, 2)
            value = lax.dot_general(kbuf[core, two, :, at].reshape(512, width), basis[lane, at], nt, preferred_element_type=F32)
            value = value.reshape(2, 256, 256)
            part[two, :, lane] = value if first else part[two, :, lane] + value
            return carry

        lax.fori_loop(0, 8, cols, 0, unroll=UNROLL)

    last = pl.ds(768, 256)

    def update_other(p, q):
        for t in range(4):
            lane = pl.ds(256 * t, 256)
            part[p, span(q), lane] += lax.dot_general(
                kbuf[1 - c, p, span(q), last], qro[lane, last], nt, preferred_element_type=F32
            )

    for k in range(CHUNKS):
        px[k].wait_send()
    back(0)
    update(0, 256, True, True)
    back(1)
    update(256, 256, True)
    for cp in kp[:4]:
        cp.wait_recv()
    update(0, 512, False)
    back(2)
    update(512, 256, True)
    for cp in kp[4:6]:
        cp.wait_recv()
    update(512, 256, False)
    back(3)
    update(768, 256, True)
    kp[6].wait_recv()
    for n, (m, q) in enumerate(pieces):
        update_other(far + order[m], q)

        @pl.when(diag)
        def _():
            ux[n].start()

        @pl.when(off)
        def _():
            uc[n].start()

        if n == 0:
            kp[7].wait_recv()
        update_other(own + order[m], q)

        @pl.when(off)
        def _():
            uy[n].start()

    @pl.when(off)
    def _():
        ya.wait_recv()

    for t in range(4):
        stat_right(own, t, True)
    for at, value in gram(y):
        lo[:, at] = BETA2 * lo[:, at] + (1.0 - BETA2) * value
    lx.wait_recv()
    lo[...] = lo[...] + (1.0 - BETA2) * lbuf[1]

    for n, (m, q) in enumerate(pieces):
        i = order[m]
        out, cols = (wt, slice(None)) if m == 0 else (wo, mine)

        @pl.when(diag)
        def _():
            uy[n].wait_recv()
            out[span(q), cols] = out[span(q), cols] - LR * (part[own + i, span(q), :] + urecv[0, i, span(q), :])

        @pl.when(off)
        def _():
            ux[n].wait_recv()
            uc[n].wait_recv()
            out[span(q), cols] = out[span(q), cols] - LR * (urecv[0, i, span(q), :] + urecv[1, i, span(q), :])

        if m == 0:
            ow[q].start()

    for cp in [*gx, gp, sm, sv, sw, qx, qya, qyb, qpa, qpb, qrp, *gf, *hx, *hc, *nx, *kp, lx]:
        cp.wait_send()

    @pl.when(diag)
    def _():
        for cp in [*y2, *y3, ya, *ux]:
            cp.wait_send()

    @pl.when(off)
    def _():
        for cp in [*f2, *f3, *uy, *uc]:
            cp.wait_send()

    for cp in (om, ov, *ow):
        cp.wait()


def _write(*refs):
    sems = refs[-1]
    count = (len(refs) - 1) // 2
    copies = []
    for n in range(count):
        rows = refs[n].shape[0]
        size = min(rows, 128)
        for lo in range(0, rows, size):
            cut = pl.ds(lo, size)
            copies.append(pltpu.make_async_copy(refs[n].at[cut, :], refs[count + n].at[cut, :], sems.at[len(copies)]))
    for cp in copies:
        cp.start()
    for cp in copies:
        cp.wait()


def solution(mesh):
    tile_spec = P(("layer", "row"), "col")

    def local_step(weight, grad_in, mom_first, mom_second, stat_left, stat_right, basis_left, basis_right):
        like = lambda a: pltpu.VMEM(a.shape, a.dtype)
        outs = pl.pallas_call(
            _step,
            out_shape=(like(weight), like(mom_first), like(mom_second), like(stat_left), like(stat_right)),
            in_specs=[pl.BlockSpec(memory_space=pl.ANY)] * 8,
            out_specs=(pl.BlockSpec(memory_space=pltpu.VMEM),) * 5,
            scratch_shapes=[
                pltpu.VMEM((2, 4, 256, 2048), F32),
                pltpu.VMEM((2, 1024, 1024), BF16),
                pltpu.VMEM((1024, 1024), BF16),
                pltpu.VMEM((4, 256, 1024), F32),
                pltpu.VMEM((4, 128, 1024), F32),
                pltpu.VMEM((4, 256, 1024), BF16),
                pltpu.VMEM((4, 256, 1024), BF16),
                pltpu.VMEM((512, 1024), BF16),
                pltpu.VMEM((256, 1024), F32),
                pltpu.VMEM((256, 1024), F32),
                pltpu.VMEM((256, 1024), F32),
                pltpu.VMEM((4, 1024, 256), BF16),
                pltpu.VMEM((2, 4, 256, 1024), BF16),
                pltpu.VMEM((2, 2, 256, 1024), F32),
                pltpu.VMEM((2, 256, 512), F32),
                pltpu.SemaphoreType.DMA((COPIES,)),
                pltpu.SemaphoreType.DMA((COPIES,)),
                pltpu.SemaphoreType.DMA((8,)),
            ],
            compiler_params=pltpu.CompilerParams(collective_id=0, has_side_effects=True, vmem_limit_bytes=GRANT),
        )(weight, grad_in, mom_first, mom_second, stat_left, stat_right, basis_left, basis_right)
        return pl.pallas_call(
            _write,
            out_shape=tuple(jax.ShapeDtypeStruct(o.shape, o.dtype) for o in outs),
            in_specs=[pl.BlockSpec(memory_space=pltpu.VMEM)] * 5,
            out_specs=(pl.BlockSpec(memory_space=pl.ANY),) * 5,
            scratch_shapes=[pltpu.SemaphoreType.DMA((16,))],
            compiler_params=pltpu.CompilerParams(vmem_limit_bytes=1048576),
        )(*(pltpu.with_memory_space_constraint(o, pltpu.VMEM) for o in outs))

    return jax.shard_map(local_step, mesh=mesh, in_specs=(tile_spec,) * 8, out_specs=(tile_spec,) * 5, check_vma=False)
```

```python
import functools

import jax
import jax.numpy as jnp
from jax import lax
from jax.experimental import pallas as pl
from jax.experimental.pallas import tpu as pltpu
from jax.sharding import PartitionSpec as P

BETA1 = 0.9
BETA2 = 0.9
EPS = 1e-8
LR = 0.1
STEP = 10
BIAS_ONE = 1.0 - BETA1 ** STEP
BIAS_TWO = 1.0 - BETA2 ** STEP

MESH = pl.DeviceIdType.MESH
F32, BF16 = jnp.float32, jnp.bfloat16
CHUNKS = 4
COPIES = 83
UNROLL = 2
GRANT = 51800000


def _step(
    w_ref, g_ref, m_ref, v_ref, l_ref, r_ref, ql_ref, qr_ref,
    wo, mo, vo, lo, acc,
    gat, qrx, qro, part, precv, hbuf, qlb, qlt, mt, vt, wt, nbuf, kbuf, urecv, lbuf,
    ssem, rsem, lsem,
):
    y, r = lax.axis_index("col"), lax.axis_index("row")
    x, c = r // 2, r % 2
    diag = x == y
    off = x != y
    sel = jnp.where(diag, 0, 1)
    own, far = 2 * x, 2 * (1 - x)
    rx = 2 * (1 - x) + c
    rp = 2 * x + 1 - c
    rxp = 2 * (1 - x) + 1 - c
    mine = pl.ds(pl.multiple_of(c * 1024, 1024), 1024)
    other = pl.ds(pl.multiple_of((1 - c) * 1024, 1024), 1024)
    to_x, to_core, to_y, to_cross = (0, y, rx), (0, y, rp), (0, 1 - y, r), (0, 1 - y, rx)

    nt = (((1,), (1,)), ((), ()))
    used = [0]
    local_used = [0]

    sends = [0]

    def remote(src, dst, dev, lane=None):
        n = used[0]
        used[0] += 1
        if lane is None:
            lane = sends[0]
            sends[0] += 1
        return pltpu.make_async_remote_copy(
            src_ref=src, dst_ref=dst, send_sem=ssem.at[lane], recv_sem=rsem.at[n], device_id=dev, device_id_type=MESH
        )

    def local(src, dst):
        n = local_used[0]
        local_used[0] += 1
        return pltpu.make_async_copy(src, dst, lsem.at[n])

    barrier = pltpu.get_barrier_semaphore()
    for dev in (to_x, to_core, to_y, to_cross):
        pl.semaphore_signal(barrier, inc=1, device_id=dev, device_id_type=MESH)

    ld_g = local(g_ref, gat.at[0, r])
    ld_qr = local(qr_ref, acc)
    ld_ql = local(ql_ref, lo)
    ld_m = local(m_ref.at[:, mine], mo.at[:, mine])
    ld_v = local(v_ref.at[:, mine], vo.at[:, mine])
    ld_w = local(w_ref.at[:, mine], wo.at[:, mine])
    for cp in (ld_ql, ld_qr, ld_g, ld_m, ld_v, ld_w):
        cp.start()

    pl.semaphore_wait(barrier, 4)

    def rows(k):
        return pl.ds(64 * k, 64)

    gx = [remote(g_ref.at[rows(k), :], gat.at[0, r, rows(k), :], to_x) for k in range(CHUNKS)]
    gp = remote(g_ref, gat.at[0, r], to_core)
    sm = remote(m_ref.at[:, other], mt, to_core)
    sv = remote(v_ref.at[:, other], vt, to_core)
    sw = remote(w_ref.at[:, other], wt, to_core)
    qcol = pl.ds(pl.multiple_of(y * 512, 512), 512)
    qx = remote(qlb.at[r, :, qcol], qlb.at[r, :, qcol], to_x)
    qya = remote(qlb.at[r, :, qcol], qlb.at[r, :, qcol], to_y)
    qyb = remote(qlb.at[rx, :, qcol], qlb.at[rx, :, qcol], to_y)
    qpa = remote(qlb.at[r], qlb.at[r], to_core)
    qpb = remote(qlb.at[rx], qlb.at[rx], to_core)
    qrp = remote(qro, qrx.at[c], to_core)
    lane = sends[0]
    gb = [remote(kbuf.at[c, pl.ds(0, 2), rows(k), :], kbuf.at[c, pl.ds(0, 2), rows(k), :], to_y) for k in range(CHUNKS)]
    fb = [remote(kbuf.at[c, pl.ds(0, 2), rows(k), :], kbuf.at[c, pl.ds(0, 2), rows(k), :], to_core, lane + k) for k in range(CHUNKS)]
    gf = [remote(gat.at[0, rx, rows(k), :], gat.at[0, rx, rows(k), :], to_core) for k in range(CHUNKS)]
    lane = sends[0]
    y2 = [remote(gat.at[0, rx, rows(k), mine], gat.at[1, rx, rows(k), mine], to_y) for k in range(CHUNKS)]
    y3 = [remote(gat.at[0, rxp, rows(k), mine], gat.at[1, rxp, rows(k), mine], to_y) for k in range(CHUNKS)]
    f2 = [remote(gat.at[1, rx, rows(k), mine], gat.at[1, rx, rows(k), mine], to_core, lane + k) for k in range(CHUNKS)]
    f3 = [remote(gat.at[1, rxp, rows(k), mine], gat.at[1, rxp, rows(k), mine], to_core, lane + 4 + k) for k in range(CHUNKS)]
    ya = remote(gat.at[0, pl.ds(own, 2), :, mine], gat.at[1, pl.ds(own, 2), :, mine], to_y)

    def pslot(base, k):
        return part.at[base + k // 2, pl.ds(128 * (k % 2), 128), :]

    px = [remote(pslot(0, k), precv.at[k], to_x) for k in range(CHUNKS)]
    hx = [remote(hbuf.at[pl.ds(own, 2), rows(k), :], hbuf.at[pl.ds(own, 2), rows(k), :], to_x) for k in range(CHUNKS - 1)]
    tail = [(pl.ds(own, 2), rows(CHUNKS - 1), pl.ds(256 * j, 256)) for j in range(4)]
    hc = [remote(hbuf.at[t], hbuf.at[t], to_x) for t in tail]
    half = pl.ds(pl.multiple_of(x * 512, 512), 512)
    nx = [remote(nbuf.at[j, half, :], nbuf.at[j, half, :], to_x) for j in range(CHUNKS)]
    kcut = [(c, pl.ds(base, 2), slice(None), pl.ds(256 * j, 256)) for j in range(CHUNKS) for base in (far, own)]
    kp = [remote(kbuf.at[cut], kbuf.at[cut], to_core) for cut in kcut]
    om = remote(mt, mo.at[:, mine], to_core)
    ov = remote(vt, vo.at[:, mine], to_core)
    order = [1 - c, c]

    def span(q):
        return pl.ds(128 * q, 128)

    ow = [remote(wt.at[span(q), :], wo.at[span(q), mine], to_core) for q in range(2)]
    pieces = [(n, q) for n in range(2) for q in range(2)]
    lane = sends[0]
    ux = [remote(part.at[far + order[n], span(q), :], urecv.at[0, order[n], span(q), :], to_x) for n, q in pieces]
    uy = [remote(part.at[own + order[n], span(q), :], urecv.at[0, order[n], span(q), :], to_y) for n, q in pieces]
    uc = [remote(part.at[far + order[n], span(q), :], urecv.at[1, order[n], span(q), :], to_cross, lane + 2 * n + q) for n, q in pieces]
    lx = remote(lbuf.at[0], lbuf.at[1], to_y)

    for cp in gx:
        cp.start()
    gp.start()
    ld_ql.wait()
    qlb[r, :, qcol] = lo[...].astype(BF16)
    ld_l = local(l_ref, lo)
    ld_l.start()
    qya.start()
    qx.start()

    ld_qr.wait()

    def to_bf(t, carry):
        span = pl.ds(pl.multiple_of(t * 128, 128), 128)
        qro[span, :] = acc[span, other].astype(BF16)
        qrx[c, span, :] = acc[span, mine].astype(BF16)
        return carry

    lax.fori_loop(0, 8, to_bf, 0)
    qrp.start()
    ld_r = local(r_ref, acc)
    ld_r.start()

    ld_g.wait()
    gp.wait_recv()

    @pl.when(diag)
    def _():
        def cast(t, carry):
            span = pl.ds(pl.multiple_of(t * 64, 64), 64)
            for i in range(2):
                for h in range(2):
                    kbuf[h, i, span, :] = gat[0, own + i, span, pl.ds(1024 * h, 1024)].astype(BF16)
            return carry

        lax.fori_loop(0, 4, cast, 0)
        gb[0].start()

    sm.start()
    sv.start()
    sw.start()

    qrp.wait_recv()

    def inner(load, store):
        lhs = [jnp.concatenate([load(0, h), load(1, h)], 0) for h in range(2)]

        def cols(t, carry):
            span = pl.ds(pl.multiple_of(t * 256, 256), 256)
            value = jnp.dot(lhs[0], qrx[0, :, span], preferred_element_type=F32)
            value += jnp.dot(lhs[1], qrx[1, :, span], preferred_element_type=F32)
            store(span, value)
            return carry

        lax.fori_loop(0, 4, cols, 0)

    def send_part(k):
        def store(span, value):
            part[k // 2, pl.ds(128 * (k % 2), 128), span] = value

        inner(lambda i, h: gat[sel, far + i, rows(k), pl.ds(1024 * h, 1024)].astype(BF16), store)
        px[k].start()

    def relay(k):
        @pl.when(off)
        def _():
            y2[k].wait_recv()
            f2[k].start()
            y3[k].wait_recv()
            f3[k].start()
            f2[k].wait_recv()
            f3[k].wait_recv()

    for k in range(CHUNKS):
        gx[k].wait_recv()
        gf[k].start()

        @pl.when(diag)
        def _():
            y2[k].start()

        gf[k].wait_recv()

        @pl.when(diag)
        def _():
            y3[k].start()

        if k == CHUNKS - 1:

            @pl.when(diag)
            def _():
                for n in range(1, CHUNKS):
                    gb[n].start()

        if k > 0:
            relay(k - 1)
            send_part(k - 1)

    qx.wait_recv()
    qyb.start()

    @pl.when(diag)
    def _():
        ya.start()

    relay(CHUNKS - 1)
    send_part(CHUNKS - 1)

    def stat_right(base, t, last):
        lane = pl.ds(pl.multiple_of(c * 1024 + t * 256, 256), 256)
        tall = jnp.concatenate([gat[sel, base, :, lane], gat[sel, base + 1, :, lane]], 0).T
        span = pl.ds(pl.multiple_of(t * 256, 256), 256)

        def cols(n, carry):
            at = pl.ds(pl.multiple_of(n * 256, 256), 256)
            wide = jnp.concatenate([gat[0, base, :, at], gat[0, base + 1, :, at]], 0)
            value = jnp.dot(tall, wide, precision=lax.Precision.HIGHEST, preferred_element_type=F32)
            prev = acc[span, at]
            if not last:
                prev = BETA2 * prev
            acc[span, at] = prev + (1.0 - BETA2) * value
            return carry

        lax.fori_loop(0, 8, cols, 0)

    def gram(k):
        for i in range(2):
            def deep(t, value, i=i):
                lane = pl.ds(pl.multiple_of(t * 256, 256), 256)
                return value + lax.dot_general(
                    gat[0, r, :, lane], gat[0, 2 * k + i, :, lane], nt, precision=lax.Precision.HIGHEST, preferred_element_type=F32
                )

            yield pl.ds(256 * i, 256), lax.fori_loop(0, 8, deep, jnp.zeros((256, 256), F32))

    ld_r.wait()
    ld_l.wait()

    def own_part(k):
        def store(span, value):
            part[2 + k // 2, pl.ds(128 * (k % 2), 128), span] = value

        inner(lambda i, h: kbuf[h, i, rows(k), :], store)

    for k in range(CHUNKS):

        @pl.when(off)
        def _():
            gb[k].wait_recv()
            fb[k].start()
            fb[k].wait_recv()

        own_part(k)
        px[k].wait_recv()
        for i in range(2):
            at = pl.ds(128 * (k % 2) + 64 * i, 64)
            hbuf[own + i, rows(k), :] = (part[2 + k // 2, at, :] + precv[k, pl.ds(64 * i, 64), :]).astype(BF16)
        if k < CHUNKS - 1:
            hx[k].start()
            stat_right(far, k, False)
    for cp in hc:
        cp.start()

    qya.wait_recv()
    qyb.wait_recv()

    @pl.when(diag)
    def _():
        for cp in gb:
            cp.wait_send()

    @pl.when(off)
    def _():
        for cp in fb:
            cp.wait_send()

    qpa.start()
    qpb.start()
    qpa.wait_recv()
    qpb.wait_recv()

    def turn(t, carry):
        lane = pl.ds(pl.multiple_of(x * 512 + t * 128, 128), 128)
        for p in range(4):
            qlt[pl.ds(pl.multiple_of(t * 128, 128), 128), pl.ds(256 * p, 256)] = qlb[p, :, lane].astype(F32).T.astype(BF16)
        return carry

    lax.fori_loop(0, 4, turn, 0)

    def basis_dot(t, base, at):
        value = jnp.zeros((128, at.size), F32)
        for i in range(2):
            lane = pl.ds(pl.multiple_of((base + i) * 256, 256), 256)
            value += jnp.dot(qlt[pl.ds(pl.multiple_of(t * 128, 128), 128), lane], hbuf[base + i, :, at], preferred_element_type=F32)
        return value

    def own_half(t, carry):
        for h in range(2):
            at = pl.ds(512 * h, 512)
            precv[t, :, at] = basis_dot(t, own, at)
        return carry

    lax.fori_loop(0, 4, own_half, 0)
    stat_right(far, 3, False)
    for at, value in gram(1 - y):
        lbuf[0, :, at] = value
    lx.start()
    ld_m.wait()
    ld_v.wait()
    ld_w.wait()
    sm.wait_recv()
    sv.wait_recv()
    sw.wait_recv()
    for cp in hx:
        cp.wait_recv()

    for j in range(CHUNKS):
        hc[j].wait_recv()
        at = pl.ds(256 * j, 256)
        lane = pl.ds(pl.multiple_of(c * 1024 + 256 * j, 256), 256)
        for n in range(2):
            i = order[n]
            mom, var, cols = (mt, vt, at) if n == 0 else (mo, vo, lane)
            for q in range(2):
                rot = precv[2 * i + q, :, at] + basis_dot(2 * i + q, far, at)
                first = BETA1 * mom[span(q), cols] + (1.0 - BETA1) * rot
                second = BETA2 * var[span(q), cols] + (1.0 - BETA2) * rot * rot
                mom[span(q), cols] = first
                var[span(q), cols] = second
                step = (first / BIAS_ONE) / (jnp.sqrt(second / BIAS_TWO) + EPS)
                nbuf[j, pl.ds(pl.multiple_of(x * 512 + 256 * i + 128 * q, 128), 128), :] = step.astype(BF16)
        nx[j].start()

    om.start()
    ov.start()

    def back(j):
        at = pl.ds(256 * j, 256)
        nx[j].wait_recv()
        for n, base in enumerate((far, own)):
            two = pl.ds(base, 2)
            value = jnp.dot(qlb[two].reshape(512, 1024), nbuf[j], preferred_element_type=F32)
            kbuf[c, two, :, at] = value.astype(BF16).reshape(2, 256, 256)
            kp[2 * j + n].start()

    def update(lo, width, near, first=False):
        at = pl.ds(lo, width)
        core, basis = (c, qrx.at[c]) if near else (1 - c, qro)

        def cols(n, carry):
            lane, two = pl.ds(pl.multiple_of(n // 2 * 256, 256), 256), pl.ds(n % 2 * 2, 2)
            value = lax.dot_general(kbuf[core, two, :, at].reshape(512, width), basis[lane, at], nt, preferred_element_type=F32)
            value = value.reshape(2, 256, 256)
            part[two, :, lane] = value if first else part[two, :, lane] + value
            return carry

        lax.fori_loop(0, 8, cols, 0, unroll=UNROLL)

    last = pl.ds(768, 256)

    def update_other(p, q):
        for t in range(4):
            lane = pl.ds(256 * t, 256)
            part[p, span(q), lane] += lax.dot_general(
                kbuf[1 - c, p, span(q), last], qro[lane, last], nt, preferred_element_type=F32
            )

    for k in range(CHUNKS):
        px[k].wait_send()
    back(0)
    update(0, 256, True, True)
    back(1)
    update(256, 256, True)
    for cp in kp[:4]:
        cp.wait_recv()
    update(0, 512, False)
    back(2)
    update(512, 256, True)
    for cp in kp[4:6]:
        cp.wait_recv()
    update(512, 256, False)
    back(3)
    update(768, 256, True)
    kp[6].wait_recv()
    for n, (m, q) in enumerate(pieces):
        update_other(far + order[m], q)

        @pl.when(diag)
        def _():
            ux[n].start()

        @pl.when(off)
        def _():
            uc[n].start()

        if n == 0:
            kp[7].wait_recv()
        update_other(own + order[m], q)

        @pl.when(off)
        def _():
            uy[n].start()

    @pl.when(off)
    def _():
        ya.wait_recv()

    for t in range(4):
        stat_right(own, t, True)
    for at, value in gram(y):
        lo[:, at] = BETA2 * lo[:, at] + (1.0 - BETA2) * value
    lx.wait_recv()
    lo[...] = lo[...] + (1.0 - BETA2) * lbuf[1]

    for n, (m, q) in enumerate(pieces):
        i = order[m]
        out, cols = (wt, slice(None)) if m == 0 else (wo, mine)

        @pl.when(diag)
        def _():
            uy[n].wait_recv()
            out[span(q), cols] = out[span(q), cols] - LR * (part[own + i, span(q), :] + urecv[0, i, span(q), :])

        @pl.when(off)
        def _():
            ux[n].wait_recv()
            uc[n].wait_recv()
            out[span(q), cols] = out[span(q), cols] - LR * (urecv[0, i, span(q), :] + urecv[1, i, span(q), :])

        if m == 0:
            ow[q].start()

    for cp in [*gx, gp, sm, sv, sw, qx, qya, qyb, qpa, qpb, qrp, *gf, *hx, *hc, *nx, *kp, lx]:
        cp.wait_send()

    @pl.when(diag)
    def _():
        for cp in [*y2, *y3, ya, *ux]:
            cp.wait_send()

    @pl.when(off)
    def _():
        for cp in [*f2, *f3, *uy, *uc]:
            cp.wait_send()

    for cp in (om, ov, *ow):
        cp.wait()


def _write(*refs):
    sems = refs[-1]
    count = (len(refs) - 1) // 2
    copies = []
    for n in range(count):
        rows = refs[n].shape[0]
        size = min(rows, 128)
        for lo in range(0, rows, size):
            cut = pl.ds(lo, size)
            copies.append(pltpu.make_async_copy(refs[n].at[cut, :], refs[count + n].at[cut, :], sems.at[len(copies)]))
    for cp in copies:
        cp.start()
    for cp in copies:
        cp.wait()


def solution(mesh):
    tile_spec = P(("layer", "row"), "col")

    def local_step(weight, grad_in, mom_first, mom_second, stat_left, stat_right, basis_left, basis_right):
        like = lambda a: pltpu.VMEM(a.shape, a.dtype)
        outs = pl.pallas_call(
            _step,
            out_shape=(like(weight), like(mom_first), like(mom_second), like(stat_left), like(stat_right)),
            in_specs=[pl.BlockSpec(memory_space=pl.ANY)] * 8,
            out_specs=(pl.BlockSpec(memory_space=pltpu.VMEM),) * 5,
            scratch_shapes=[
                pltpu.VMEM((2, 4, 256, 2048), F32),
                pltpu.VMEM((2, 1024, 1024), BF16),
                pltpu.VMEM((1024, 1024), BF16),
                pltpu.VMEM((4, 256, 1024), F32),
                pltpu.VMEM((4, 128, 1024), F32),
                pltpu.VMEM((4, 256, 1024), BF16),
                pltpu.VMEM((4, 256, 1024), BF16),
                pltpu.VMEM((512, 1024), BF16),
                pltpu.VMEM((256, 1024), F32),
                pltpu.VMEM((256, 1024), F32),
                pltpu.VMEM((256, 1024), F32),
                pltpu.VMEM((4, 1024, 256), BF16),
                pltpu.VMEM((2, 4, 256, 1024), BF16),
                pltpu.VMEM((2, 2, 256, 1024), F32),
                pltpu.VMEM((2, 256, 512), F32),
                pltpu.SemaphoreType.DMA((COPIES - 16,)),
                pltpu.SemaphoreType.DMA((COPIES,)),
                pltpu.SemaphoreType.DMA((8,)),
            ],
            compiler_params=pltpu.CompilerParams(collective_id=0, has_side_effects=True, vmem_limit_bytes=GRANT),
        )(weight, grad_in, mom_first, mom_second, stat_left, stat_right, basis_left, basis_right)
        return pl.pallas_call(
            _write,
            out_shape=tuple(jax.ShapeDtypeStruct(o.shape, o.dtype) for o in outs),
            in_specs=[pl.BlockSpec(memory_space=pltpu.VMEM)] * 5,
            out_specs=(pl.BlockSpec(memory_space=pl.ANY),) * 5,
            scratch_shapes=[pltpu.SemaphoreType.DMA((16,))],
            compiler_params=pltpu.CompilerParams(vmem_limit_bytes=1048576),
        )(*(pltpu.with_memory_space_constraint(o, pltpu.VMEM) for o in outs))

    return jax.shard_map(local_step, mesh=mesh, in_specs=(tile_spec,) * 8, out_specs=(tile_spec,) * 5, check_vma=False)
```

```python
import functools

import jax
import jax.numpy as jnp
from jax import lax
from jax.experimental import pallas as pl
from jax.experimental.pallas import tpu as pltpu
from jax.sharding import PartitionSpec as P

BETA1 = 0.9
BETA2 = 0.9
EPS = 1e-8
LR = 0.1
STEP = 10
BIAS_ONE = 1.0 - BETA1 ** STEP
BIAS_TWO = 1.0 - BETA2 ** STEP

MESH = pl.DeviceIdType.MESH
F32, BF16 = jnp.float32, jnp.bfloat16
CHUNKS = 4
COPIES = 83
UNROLL = 2
GRANT = 51800000


def _step(
    w_ref, g_ref, m_ref, v_ref, l_ref, r_ref, ql_ref, qr_ref,
    wo, mo, vo, lo, acc,
    gat, qrx, qro, part, precv, hbuf, qlb, qlt, mt, vt, wt, nbuf, kbuf, urecv, lbuf,
    ssem, rsem, lsem,
):
    y, r = lax.axis_index("col"), lax.axis_index("row")
    x, c = r // 2, r % 2
    diag = x == y
    off = x != y
    sel = jnp.where(diag, 0, 1)
    own, far = 2 * x, 2 * (1 - x)
    rx = 2 * (1 - x) + c
    rp = 2 * x + 1 - c
    rxp = 2 * (1 - x) + 1 - c
    mine = pl.ds(pl.multiple_of(c * 1024, 1024), 1024)
    other = pl.ds(pl.multiple_of((1 - c) * 1024, 1024), 1024)
    to_x, to_core, to_y, to_cross = (0, y, rx), (0, y, rp), (0, 1 - y, r), (0, 1 - y, rx)

    nt = (((1,), (1,)), ((), ()))
    used = [0]
    local_used = [0]

    sends = [0]

    def remote(src, dst, dev, lane=None):
        n = used[0]
        used[0] += 1
        if lane is None:
            lane = sends[0]
            sends[0] += 1
        return pltpu.make_async_remote_copy(
            src_ref=src, dst_ref=dst, send_sem=ssem.at[lane], recv_sem=rsem.at[n], device_id=dev, device_id_type=MESH
        )

    def local(src, dst):
        n = local_used[0]
        local_used[0] += 1
        return pltpu.make_async_copy(src, dst, lsem.at[n])

    barrier = pltpu.get_barrier_semaphore()
    for dev in (to_x, to_core, to_y, to_cross):
        pl.semaphore_signal(barrier, inc=1, device_id=dev, device_id_type=MESH)

    ld_g = local(g_ref, gat.at[0, r])
    ld_qr = local(qr_ref, acc)
    ld_ql = local(ql_ref, lo)
    ld_m = local(m_ref.at[:, mine], mo.at[:, mine])
    ld_v = local(v_ref.at[:, mine], vo.at[:, mine])
    ld_w = local(w_ref.at[:, mine], wo.at[:, mine])
    for cp in (ld_ql, ld_qr, ld_g, ld_m, ld_v, ld_w):
        cp.start()

    pl.semaphore_wait(barrier, 4)

    def rows(k):
        return pl.ds(64 * k, 64)

    lane = sends[0]
    sends[0] += 1
    gx = [remote(g_ref.at[rows(k), :], gat.at[0, r, rows(k), :], to_x, lane) for k in range(CHUNKS)]
    gx_all = pltpu.make_async_remote_copy(
        src_ref=g_ref, dst_ref=gat.at[0, r], send_sem=ssem.at[lane], recv_sem=rsem.at[0], device_id=to_x, device_id_type=MESH
    )
    gp = remote(g_ref, gat.at[0, r], to_core)
    sm = remote(m_ref.at[:, other], mt, to_core)
    sv = remote(v_ref.at[:, other], vt, to_core)
    sw = remote(w_ref.at[:, other], wt, to_core)
    qcol = pl.ds(pl.multiple_of(y * 512, 512), 512)
    qx = remote(qlb.at[r, :, qcol], qlb.at[r, :, qcol], to_x)
    qya = remote(qlb.at[r, :, qcol], qlb.at[r, :, qcol], to_y)
    qyb = remote(qlb.at[rx, :, qcol], qlb.at[rx, :, qcol], to_y)
    qpa = remote(qlb.at[r], qlb.at[r], to_core)
    qpb = remote(qlb.at[rx], qlb.at[rx], to_core)
    qrp = remote(qro, qrx.at[c], to_core)
    lane = sends[0]
    gb = [remote(kbuf.at[c, pl.ds(0, 2), rows(k), :], kbuf.at[c, pl.ds(0, 2), rows(k), :], to_y) for k in range(CHUNKS)]
    fb = [remote(kbuf.at[c, pl.ds(0, 2), rows(k), :], kbuf.at[c, pl.ds(0, 2), rows(k), :], to_core, lane + k) for k in range(CHUNKS)]
    gf = [remote(gat.at[0, rx, rows(k), :], gat.at[0, rx, rows(k), :], to_core) for k in range(CHUNKS)]
    lane = sends[0]
    y2 = [remote(gat.at[0, rx, rows(k), mine], gat.at[1, rx, rows(k), mine], to_y) for k in range(CHUNKS)]
    y3 = [remote(gat.at[0, rxp, rows(k), mine], gat.at[1, rxp, rows(k), mine], to_y) for k in range(CHUNKS)]
    f2 = [remote(gat.at[1, rx, rows(k), mine], gat.at[1, rx, rows(k), mine], to_core, lane + k) for k in range(CHUNKS)]
    f3 = [remote(gat.at[1, rxp, rows(k), mine], gat.at[1, rxp, rows(k), mine], to_core, lane + 4 + k) for k in range(CHUNKS)]
    ya = remote(gat.at[0, pl.ds(own, 2), :, mine], gat.at[1, pl.ds(own, 2), :, mine], to_y)

    def pslot(base, k):
        return part.at[base + k // 2, pl.ds(128 * (k % 2), 128), :]

    px = [remote(pslot(0, k), precv.at[k], to_x) for k in range(CHUNKS)]
    hx = [remote(hbuf.at[pl.ds(own, 2), rows(k), :], hbuf.at[pl.ds(own, 2), rows(k), :], to_x) for k in range(CHUNKS - 1)]
    tail = [(pl.ds(own, 2), rows(CHUNKS - 1), pl.ds(256 * j, 256)) for j in range(4)]
    hc = [remote(hbuf.at[t], hbuf.at[t], to_x) for t in tail]
    half = pl.ds(pl.multiple_of(x * 512, 512), 512)
    nx = [remote(nbuf.at[j, half, :], nbuf.at[j, half, :], to_x) for j in range(CHUNKS)]
    kcut = [(c, pl.ds(base, 2), slice(None), pl.ds(256 * j, 256)) for j in range(CHUNKS) for base in (far, own)]
    kp = [remote(kbuf.at[cut], kbuf.at[cut], to_core) for cut in kcut]
    om = remote(mt, mo.at[:, mine], to_core)
    ov = remote(vt, vo.at[:, mine], to_core)
    order = [1 - c, c]

    def span(q):
        return pl.ds(128 * q, 128)

    ow = [remote(wt.at[span(q), :], wo.at[span(q), mine], to_core) for q in range(2)]
    pieces = [(n, q) for n in range(2) for q in range(2)]
    lane = sends[0]
    ux = [remote(part.at[far + order[n], span(q), :], urecv.at[0, order[n], span(q), :], to_x) for n, q in pieces]
    uy = [remote(part.at[own + order[n], span(q), :], urecv.at[0, order[n], span(q), :], to_y) for n, q in pieces]
    uc = [remote(part.at[far + order[n], span(q), :], urecv.at[1, order[n], span(q), :], to_cross, lane + 2 * n + q) for n, q in pieces]
    lx = remote(lbuf.at[0], lbuf.at[1], to_y)

    for cp in gx:
        cp.start()
    gp.start()
    ld_ql.wait()
    qlb[r, :, qcol] = lo[...].astype(BF16)
    ld_l = local(l_ref, lo)
    ld_l.start()
    qya.start()
    qx.start()

    ld_qr.wait()

    def to_bf(t, carry):
        span = pl.ds(pl.multiple_of(t * 128, 128), 128)
        qro[span, :] = acc[span, other].astype(BF16)
        qrx[c, span, :] = acc[span, mine].astype(BF16)
        return carry

    lax.fori_loop(0, 8, to_bf, 0)
    qrp.start()
    ld_r = local(r_ref, acc)
    ld_r.start()

    ld_g.wait()
    gp.wait_recv()

    @pl.when(diag)
    def _():
        def cast(t, carry):
            span = pl.ds(pl.multiple_of(t * 64, 64), 64)
            for i in range(2):
                for h in range(2):
                    kbuf[h, i, span, :] = gat[0, own + i, span, pl.ds(1024 * h, 1024)].astype(BF16)
            return carry

        lax.fori_loop(0, 4, cast, 0)
        gb[0].start()

    sm.start()
    sv.start()
    sw.start()

    qrp.wait_recv()

    def inner(load, store):
        lhs = [jnp.concatenate([load(0, h), load(1, h)], 0) for h in range(2)]

        def cols(t, carry):
            span = pl.ds(pl.multiple_of(t * 256, 256), 256)
            value = jnp.dot(lhs[0], qrx[0, :, span], preferred_element_type=F32)
            value += jnp.dot(lhs[1], qrx[1, :, span], preferred_element_type=F32)
            store(span, value)
            return carry

        lax.fori_loop(0, 4, cols, 0)

    def send_part(k):
        def store(span, value):
            part[k // 2, pl.ds(128 * (k % 2), 128), span] = value

        inner(lambda i, h: gat[sel, far + i, rows(k), pl.ds(1024 * h, 1024)].astype(BF16), store)
        px[k].start()

    def relay(k):
        @pl.when(off)
        def _():
            y2[k].wait_recv()
            f2[k].start()
            y3[k].wait_recv()
            f3[k].start()
            f2[k].wait_recv()
            f3[k].wait_recv()

    for k in range(CHUNKS):
        gx[k].wait_recv()
        gf[k].start()

        @pl.when(diag)
        def _():
            y2[k].start()

        gf[k].wait_recv()

        @pl.when(diag)
        def _():
            y3[k].start()

        if k == CHUNKS - 1:

            @pl.when(diag)
            def _():
                for n in range(1, CHUNKS):
                    gb[n].start()

        if k > 0:
            relay(k - 1)
            send_part(k - 1)

    qx.wait_recv()
    qyb.start()

    @pl.when(diag)
    def _():
        ya.start()

    relay(CHUNKS - 1)
    send_part(CHUNKS - 1)

    def stat_right(base, t, last):
        lane = pl.ds(pl.multiple_of(c * 1024 + t * 256, 256), 256)
        tall = jnp.concatenate([gat[sel, base, :, lane], gat[sel, base + 1, :, lane]], 0).T
        span = pl.ds(pl.multiple_of(t * 256, 256), 256)

        def cols(n, carry):
            at = pl.ds(pl.multiple_of(n * 256, 256), 256)
            wide = jnp.concatenate([gat[0, base, :, at], gat[0, base + 1, :, at]], 0)
            value = jnp.dot(tall, wide, precision=lax.Precision.HIGHEST, preferred_element_type=F32)
            prev = acc[span, at]
            if not last:
                prev = BETA2 * prev
            acc[span, at] = prev + (1.0 - BETA2) * value
            return carry

        lax.fori_loop(0, 8, cols, 0)

    def gram(k):
        for i in range(2):
            def deep(t, value, i=i):
                lane = pl.ds(pl.multiple_of(t * 256, 256), 256)
                return value + lax.dot_general(
                    gat[0, r, :, lane], gat[0, 2 * k + i, :, lane], nt, precision=lax.Precision.HIGHEST, preferred_element_type=F32
                )

            yield pl.ds(256 * i, 256), lax.fori_loop(0, 8, deep, jnp.zeros((256, 256), F32))

    ld_r.wait()
    ld_l.wait()

    def own_part(k):
        def store(span, value):
            part[2 + k // 2, pl.ds(128 * (k % 2), 128), span] = value

        inner(lambda i, h: kbuf[h, i, rows(k), :], store)

    for k in range(CHUNKS):

        @pl.when(off)
        def _():
            gb[k].wait_recv()
            fb[k].start()
            fb[k].wait_recv()

        own_part(k)
        px[k].wait_recv()
        for i in range(2):
            at = pl.ds(128 * (k % 2) + 64 * i, 64)
            hbuf[own + i, rows(k), :] = (part[2 + k // 2, at, :] + precv[k, pl.ds(64 * i, 64), :]).astype(BF16)
        if k < CHUNKS - 1:
            hx[k].start()
            stat_right(far, k, False)
    for cp in hc:
        cp.start()

    qya.wait_recv()
    qyb.wait_recv()

    @pl.when(diag)
    def _():
        for cp in gb:
            cp.wait_send()

    @pl.when(off)
    def _():
        for cp in fb:
            cp.wait_send()

    qpa.start()
    qpb.start()
    qpa.wait_recv()
    qpb.wait_recv()

    def turn(t, carry):
        lane = pl.ds(pl.multiple_of(x * 512 + t * 128, 128), 128)
        for p in range(4):
            qlt[pl.ds(pl.multiple_of(t * 128, 128), 128), pl.ds(256 * p, 256)] = qlb[p, :, lane].astype(F32).T.astype(BF16)
        return carry

    lax.fori_loop(0, 4, turn, 0)

    def basis_dot(t, base, at):
        value = jnp.zeros((128, at.size), F32)
        for i in range(2):
            lane = pl.ds(pl.multiple_of((base + i) * 256, 256), 256)
            value += jnp.dot(qlt[pl.ds(pl.multiple_of(t * 128, 128), 128), lane], hbuf[base + i, :, at], preferred_element_type=F32)
        return value

    def own_half(t, carry):
        for h in range(2):
            at = pl.ds(512 * h, 512)
            precv[t, :, at] = basis_dot(t, own, at)
        return carry

    lax.fori_loop(0, 4, own_half, 0)
    stat_right(far, 3, False)
    for at, value in gram(1 - y):
        lbuf[0, :, at] = value
    lx.start()
    ld_m.wait()
    ld_v.wait()
    ld_w.wait()
    sm.wait_recv()
    sv.wait_recv()
    sw.wait_recv()
    for cp in hx:
        cp.wait_recv()

    for j in range(CHUNKS):
        hc[j].wait_recv()
        at = pl.ds(256 * j, 256)
        lane = pl.ds(pl.multiple_of(c * 1024 + 256 * j, 256), 256)
        for n in range(2):
            i = order[n]
            mom, var, cols = (mt, vt, at) if n == 0 else (mo, vo, lane)
            for q in range(2):
                rot = precv[2 * i + q, :, at] + basis_dot(2 * i + q, far, at)
                first = BETA1 * mom[span(q), cols] + (1.0 - BETA1) * rot
                second = BETA2 * var[span(q), cols] + (1.0 - BETA2) * rot * rot
                mom[span(q), cols] = first
                var[span(q), cols] = second
                step = (first / BIAS_ONE) / (jnp.sqrt(second / BIAS_TWO) + EPS)
                nbuf[j, pl.ds(pl.multiple_of(x * 512 + 256 * i + 128 * q, 128), 128), :] = step.astype(BF16)
        nx[j].start()

    om.start()
    ov.start()

    def back(j):
        at = pl.ds(256 * j, 256)
        nx[j].wait_recv()
        for n, base in enumerate((far, own)):
            two = pl.ds(base, 2)
            value = jnp.dot(qlb[two].reshape(512, 1024), nbuf[j], preferred_element_type=F32)
            kbuf[c, two, :, at] = value.astype(BF16).reshape(2, 256, 256)
            kp[2 * j + n].start()

    def update(lo, width, near, first=False):
        at = pl.ds(lo, width)
        core, basis = (c, qrx.at[c]) if near else (1 - c, qro)

        def cols(n, carry):
            lane, two = pl.ds(pl.multiple_of(n // 2 * 256, 256), 256), pl.ds(n % 2 * 2, 2)
            value = lax.dot_general(kbuf[core, two, :, at].reshape(512, width), basis[lane, at], nt, preferred_element_type=F32)
            value = value.reshape(2, 256, 256)
            part[two, :, lane] = value if first else part[two, :, lane] + value
            return carry

        lax.fori_loop(0, 8, cols, 0, unroll=UNROLL)

    last = pl.ds(768, 256)

    def update_other(p, q):
        for t in range(4):
            lane = pl.ds(256 * t, 256)
            part[p, span(q), lane] += lax.dot_general(
                kbuf[1 - c, p, span(q), last], qro[lane, last], nt, preferred_element_type=F32
            )

    for k in range(CHUNKS):
        px[k].wait_send()
    back(0)
    update(0, 256, True, True)
    back(1)
    update(256, 256, True)
    for cp in kp[:4]:
        cp.wait_recv()
    update(0, 512, False)
    back(2)
    update(512, 256, True)
    for cp in kp[4:6]:
        cp.wait_recv()
    update(512, 256, False)
    back(3)
    update(768, 256, True)
    kp[6].wait_recv()
    for n, (m, q) in enumerate(pieces):
        update_other(far + order[m], q)

        @pl.when(diag)
        def _():
            ux[n].start()

        @pl.when(off)
        def _():
            uc[n].start()

        if n == 0:
            kp[7].wait_recv()
        update_other(own + order[m], q)

        @pl.when(off)
        def _():
            uy[n].start()

    @pl.when(off)
    def _():
        ya.wait_recv()

    for t in range(4):
        stat_right(own, t, True)
    for at, value in gram(y):
        lo[:, at] = BETA2 * lo[:, at] + (1.0 - BETA2) * value
    lx.wait_recv()
    lo[...] = lo[...] + (1.0 - BETA2) * lbuf[1]

    for n, (m, q) in enumerate(pieces):
        i = order[m]
        out, cols = (wt, slice(None)) if m == 0 else (wo, mine)

        @pl.when(diag)
        def _():
            uy[n].wait_recv()
            out[span(q), cols] = out[span(q), cols] - LR * (part[own + i, span(q), :] + urecv[0, i, span(q), :])

        @pl.when(off)
        def _():
            ux[n].wait_recv()
            uc[n].wait_recv()
            out[span(q), cols] = out[span(q), cols] - LR * (urecv[0, i, span(q), :] + urecv[1, i, span(q), :])

        if m == 0:
            ow[q].start()

    for cp in [gx_all, gp, sm, sv, sw, qx, qya, qyb, qpa, qpb, qrp, *gf, *hx, *hc, *nx, *kp, lx]:
        cp.wait_send()

    @pl.when(diag)
    def _():
        for cp in [*y2, *y3, ya, *ux]:
            cp.wait_send()

    @pl.when(off)
    def _():
        for cp in [*f2, *f3, *uy, *uc]:
            cp.wait_send()

    for cp in (om, ov, *ow):
        cp.wait()


def _write(*refs):
    sems = refs[-1]
    count = (len(refs) - 1) // 2
    copies = []
    for n in range(count):
        rows = refs[n].shape[0]
        size = min(rows, 128)
        for lo in range(0, rows, size):
            cut = pl.ds(lo, size)
            copies.append(pltpu.make_async_copy(refs[n].at[cut, :], refs[count + n].at[cut, :], sems.at[len(copies)]))
    for cp in copies:
        cp.start()
    for cp in copies:
        cp.wait()


def solution(mesh):
    tile_spec = P(("layer", "row"), "col")

    def local_step(weight, grad_in, mom_first, mom_second, stat_left, stat_right, basis_left, basis_right):
        like = lambda a: pltpu.VMEM(a.shape, a.dtype)
        outs = pl.pallas_call(
            _step,
            out_shape=(like(weight), like(mom_first), like(mom_second), like(stat_left), like(stat_right)),
            in_specs=[pl.BlockSpec(memory_space=pl.ANY)] * 8,
            out_specs=(pl.BlockSpec(memory_space=pltpu.VMEM),) * 5,
            scratch_shapes=[
                pltpu.VMEM((2, 4, 256, 2048), F32),
                pltpu.VMEM((2, 1024, 1024), BF16),
                pltpu.VMEM((1024, 1024), BF16),
                pltpu.VMEM((4, 256, 1024), F32),
                pltpu.VMEM((4, 128, 1024), F32),
                pltpu.VMEM((4, 256, 1024), BF16),
                pltpu.VMEM((4, 256, 1024), BF16),
                pltpu.VMEM((512, 1024), BF16),
                pltpu.VMEM((256, 1024), F32),
                pltpu.VMEM((256, 1024), F32),
                pltpu.VMEM((256, 1024), F32),
                pltpu.VMEM((4, 1024, 256), BF16),
                pltpu.VMEM((2, 4, 256, 1024), BF16),
                pltpu.VMEM((2, 2, 256, 1024), F32),
                pltpu.VMEM((2, 256, 512), F32),
                pltpu.SemaphoreType.DMA((COPIES - 19,)),
                pltpu.SemaphoreType.DMA((COPIES,)),
                pltpu.SemaphoreType.DMA((8,)),
            ],
            compiler_params=pltpu.CompilerParams(collective_id=0, has_side_effects=True, vmem_limit_bytes=GRANT),
        )(weight, grad_in, mom_first, mom_second, stat_left, stat_right, basis_left, basis_right)
        return pl.pallas_call(
            _write,
            out_shape=tuple(jax.ShapeDtypeStruct(o.shape, o.dtype) for o in outs),
            in_specs=[pl.BlockSpec(memory_space=pltpu.VMEM)] * 5,
            out_specs=(pl.BlockSpec(memory_space=pl.ANY),) * 5,
            scratch_shapes=[pltpu.SemaphoreType.DMA((16,))],
            compiler_params=pltpu.CompilerParams(vmem_limit_bytes=1048576),
        )(*(pltpu.with_memory_space_constraint(o, pltpu.VMEM) for o in outs))

    return jax.shard_map(local_step, mesh=mesh, in_specs=(tile_spec,) * 8, out_specs=(tile_spec,) * 5, check_vma=False)
```
